32 devices in a mesh: vert: 8 (over z, y), col: 4 (over x, core).
Axes of the slice: x: 2, y: 2, z: 4, core: 2. Of those that a mesh axis runs over, the one named last changes fastest.
Arguments:
- coeffs: bfloat16 [64, 400], P(('vert', 'col')), may hold values from -6 to 6
- shape_basis: bfloat16 [400, 3, 656], P('col', None, 'vert'), may hold values from -0.3125 to 0.3125
- template: float32 [3, 656], P(None, 'vert'), may hold values from -6 to 6
- regressor: float32 [55, 656], P(None, 'vert'), may hold values from -0.5 to 0.5
- quaternions: float32 [64, 4, 55], P(('vert', 'col')), may hold values from -1.5 to 1.5, as said below
- translation: float32 [64, 3], P(('vert', 'col')), may hold values from -6 to 6
- parents: int32 [55], replicated, may hold values from 0 to 53, as said below
- skin_index: int32 [656, 4], P('vert'), may hold values from 0 to 54, all different within a row
- skin_raw: float32 [656, 4], P('vert'), may hold values from 0.1 to 1
Outputs:
- posed_vertices: bfloat16 [64, 3, 656], P(('vert', 'col'))
The draws below stay inside these ranges and needn't reach their ends.
Inputs may be any that keep to these rules, and one draw needn't show every extreme that they name: parents[0] = 0 and parents[j] < j for j >= 1. `skin_index`: the four joints of a vertex differ. `quaternions`: component 0 lies in [0.5, 1.5].
All inputs are finite; a program needn't handle non-finite values.
Results may differ from the reference program's by a relative error of at most 0.0024.
Values may be sent and summed in bfloat16 or wider, within the bound.
No kernel may reach another device: no remote copies, remote signals or barrier semaphores. Data moves between devices by JAX's collectives and lax.ppermute only.
A program may use at most 64 MiB of HBM per device.

```python
import math
import jax
import jax.numpy as jnp
from jax import lax

K = 400
J = 55
V = 656
CHARS = 64
N_VERT = 8


def draw_quaternions(key, part):
    first_key = jax.random.fold_in(key, 11)
    second_key = jax.random.fold_in(key, 12)
    scalar_part = jax.random.uniform(first_key, (CHARS, 1, J), jnp.float32, 0.75, 1.25)
    vector_part = jnp.clip(0.4 * jax.random.normal(second_key, (CHARS, 3, J), jnp.float32), -1.5, 1.5)
    return jnp.concatenate([scalar_part, vector_part], axis=1)


def draw_parents(key, part):
    steps_back = jax.random.randint(jax.random.fold_in(key, 21), (J,), 0, 3)
    joint_ids = jnp.arange(J, dtype=jnp.int32)
    return jnp.maximum(joint_ids - 1 - steps_back, 0).astype(jnp.int32)


def level_of(own_key, shape, split, smallest, largest):
    factor_of = 1.0
    for dim, parts in split:
        draws = jax.random.uniform(jax.random.fold_in(jax.random.fold_in(own_key, 6), dim), (parts,), jnp.float32, smallest / len(split), largest / len(split))
        factor_of = factor_of * jnp.repeat(jnp.exp(draws), shape[dim] // parts).reshape((-1,) + (1,) * (len(shape) - 1 - dim))
    return factor_of


def picks_of(key, rows, count, top, lift):
    order = jax.random.permutation(jax.random.fold_in(key, 1), count)
    favour = order
    for power in range(3):
        favour = favour * favour // count
    favour = favour * lift // count
    tickets = jax.random.randint(jax.random.fold_in(key, 2), (rows, count), 0, 4096) + favour
    fixed_rows = jax.random.permutation(jax.random.fold_in(key, 3), rows)[jnp.arange(count) % rows]
    tickets = jnp.where(jnp.arange(rows)[:, None] == fixed_rows[None, :], 1 << 14, tickets)
    priority = tickets * count + jnp.arange(count)
    return lax.top_k(priority.astype(jnp.int32), top)[1].astype(jnp.int32)


def centred(own_key, shape, spread, bound, shards=(), kind=jnp.bfloat16):
    entries = spread * jax.random.normal(own_key, shape, jnp.float32)
    if shards:
        entries = entries * level_of(own_key, shape, shards, -0.22, 0.18)
    return jnp.clip(entries, -bound, bound).astype(kind)


def setup_inputs(seed: int = 0) -> dict:
    seeds = jax.random.split(jax.random.key(seed), 10)
    coeffs = centred(seeds[0], (CHARS, K), 1.0, 6.0, ((0, 32),))
    shape_basis = centred(seeds[1], (K, 3, V), K ** -0.5, 0.3125, ((0, 4), (2, 8)))
    template = centred(seeds[2], (3, V), 1.0, 6.0, ((1, 8),), jnp.float32)
    regressor = centred(seeds[3], (J, V), (V // 4) ** -0.5, 0.5, ((1, 8),), jnp.float32)
    quaternions = draw_quaternions(jax.random.fold_in(seeds[9], 71), 0)
    translation = centred(seeds[5], (CHARS, 3), 1.0, 6.0, ((0, 32),), jnp.float32)
    parents = draw_parents(jax.random.fold_in(seeds[9], 71), 0)
    skin_index = picks_of(seeds[7], V, J, 4, 595)
    skin_raw = jnp.clip(jnp.exp(math.log(1.0) - 2.3025851 * jax.random.uniform(seeds[8], (V, 4), jnp.float32) ** level_of(seeds[8], (V, 4), ((0, 8),), -0.2, 0.2)), 0.1, 1.0)
    return dict(coeffs=coeffs, shape_basis=shape_basis, template=template, regressor=regressor, quaternions=quaternions, translation=translation, parents=parents, skin_index=skin_index, skin_raw=skin_raw)


def rotations(quaternions):
    quat_w = jnp.transpose(quaternions[:, 0])
    quat_x = jnp.transpose(quaternions[:, 1])
    quat_y = jnp.transpose(quaternions[:, 2])
    quat_z = jnp.transpose(quaternions[:, 3])
    scale_two = 2.0 / (quat_w * quat_w + quat_x * quat_x + quat_y * quat_y + quat_z * quat_z)
    matrix_rows = [
        [1.0 - scale_two * (quat_y * quat_y + quat_z * quat_z), scale_two * (quat_x * quat_y - quat_w * quat_z), scale_two * (quat_x * quat_z + quat_w * quat_y)],
        [scale_two * (quat_x * quat_y + quat_w * quat_z), 1.0 - scale_two * (quat_x * quat_x + quat_z * quat_z), scale_two * (quat_y * quat_z - quat_w * quat_x)],
        [scale_two * (quat_x * quat_z - quat_w * quat_y), scale_two * (quat_y * quat_z + quat_w * quat_x), 1.0 - scale_two * (quat_x * quat_x + quat_y * quat_y)],
    ]
    return jnp.stack([jnp.stack(entry, axis=1) for entry in matrix_rows], axis=1)


def kinematics(joints, quaternions, translation, parents):
    joint_total = quaternions.shape[2]
    local_rots = rotations(quaternions)
    places = jnp.transpose(joints, (2, 1, 0))
    glob_rot = jnp.zeros_like(local_rots).at[0].set(local_rots[0])
    glob_pos = jnp.zeros_like(places).at[0].set(places[0] + jnp.transpose(translation))

    def compose(joint, state_pair):
        rot_now, pos_now = state_pair
        parent = lax.dynamic_index_in_dim(parents, joint, 0, keepdims=False)
        parent_rot = lax.dynamic_index_in_dim(rot_now, parent, 0, keepdims=False)
        parent_pos = lax.dynamic_index_in_dim(pos_now, parent, 0, keepdims=False)
        local_rot = lax.dynamic_index_in_dim(local_rots, joint, 0, keepdims=False)
        offset = lax.dynamic_index_in_dim(places, joint, 0, keepdims=False) - lax.dynamic_index_in_dim(places, parent, 0, keepdims=False)
        new_rot = jnp.einsum("amc,mbc->abc", parent_rot, local_rot, precision=lax.Precision.HIGHEST)
        new_pos = jnp.einsum("amc,mc->ac", parent_rot, offset, precision=lax.Precision.HIGHEST) + parent_pos
        rot_now = lax.dynamic_update_index_in_dim(rot_now, new_rot, joint, 0)
        pos_now = lax.dynamic_update_index_in_dim(pos_now, new_pos, joint, 0)
        return (rot_now, pos_now)

    glob_rot, glob_pos = lax.fori_loop(1, joint_total, compose, (glob_rot, glob_pos))
    correction = glob_pos - jnp.einsum("jamc,jmc->jac", glob_rot, places, precision=lax.Precision.HIGHEST)
    frames = jnp.concatenate([glob_rot.reshape(joint_total, 9, glob_rot.shape[3]), correction], axis=1)
    return jnp.transpose(frames, (2, 1, 0))


def dense_weights(joint_index, raw_weights, joint_total):
    shares = raw_weights / jnp.sum(raw_weights, axis=1, keepdims=True)
    matches = joint_index[None, :, :] == jnp.arange(joint_total, dtype=jnp.int32)[:, None, None]
    return jnp.sum(jnp.where(matches, shares[None, :, :], jnp.zeros_like(shares)[None, :, :]), axis=2)


def apply_frames(blended, shaped_wide):
    coords = []
    for axis_out in range(3):
        value = blended[:, 9 + axis_out]
        for axis_in in range(3):
            value = value + blended[:, 3 * axis_out + axis_in] * shaped_wide[:, axis_in]
        coords.append(value)
    return jnp.stack(coords, axis=1)


def reference(coeffs, shape_basis, template, regressor, quaternions, translation, parents, skin_index, skin_raw):
    components = shape_basis.shape[0]
    vert_total = shape_basis.shape[2]
    flat_basis = shape_basis.reshape(components, 3 * vert_total)
    base_row = template.reshape(1, 3 * vert_total)
    weight_grid = dense_weights(skin_index, skin_raw, J)
    basis_table = jnp.einsum("kmv,jv->kmj", shape_basis.astype(jnp.float32), regressor, precision=lax.Precision.HIGHEST)
    base_table = jnp.einsum("mv,jv->mj", template, regressor, precision=lax.Precision.HIGHEST)
    block_size = CHARS // N_VERT

    def block_pass(inputs):
        coeff_block, quat_block, shift_block = inputs
        shaped = (jnp.dot(coeff_block, flat_basis, preferred_element_type=jnp.float32) + base_row).astype(jnp.bfloat16)
        shaped_wide = shaped.reshape(block_size, 3, vert_total).astype(jnp.float32)
        joints = jnp.einsum("ck,kmj->cmj", coeff_block.astype(jnp.float32), basis_table, precision=lax.Precision.HIGHEST) + base_table[None]
        frames = kinematics(joints, quat_block, shift_block, parents)
        blended = jnp.einsum("cej,jv->cev", frames, weight_grid, precision=lax.Precision.HIGHEST)
        return apply_frames(blended, shaped_wide).astype(jnp.bfloat16)

    result = lax.map(block_pass, (coeffs.reshape(N_VERT, block_size, components), quaternions.reshape(N_VERT, block_size, 4, J), translation.reshape(N_VERT, block_size, 3)))
    return result.reshape(CHARS, 3, vert_total)
```

```python
import functools

import jax
import jax.numpy as jnp
from jax import lax
from jax.experimental import pallas as pl
from jax.experimental.pallas import tpu as pltpu
from jax.sharding import PartitionSpec as P

LANES = 128
SUBS = 8
VMEM = pl.BlockSpec(memory_space=pltpu.VMEM)


def round_up(value, step):
    return -(-value // step) * step


def pack_kernel(groups, spans, slots, coeffs_ref, index_ref, raw_ref, out_ref):
    own_chars, comps = coeffs_ref.shape
    block = comps // groups
    verts = index_ref.shape[1]
    rows = out_ref.shape[1]
    column = lax.axis_index("col")
    wide = coeffs_ref[...].astype(jnp.float32)
    index = index_ref[...].astype(jnp.float32)
    raw = raw_ref[...]
    out_ref[...] = jnp.zeros_like(out_ref)
    per_group = slots // groups
    picked = []
    for which in range(per_group):
        slot = column * per_group + which
        sel = lax.broadcasted_iota(jnp.int32, index.shape, 0) == slot
        picked.append(jnp.sum(jnp.where(sel, index, 0.0), axis=0, keepdims=True))
        picked.append(jnp.sum(jnp.where(sel, raw, 0.0), axis=0, keepdims=True))
    for group in range(groups):
        piece = wide[:, group * block : (group + 1) * block]
        for span in range(spans):
            out_ref[span * groups + group, 0:own_chars, 0:block] = piece
            for row, value in enumerate(picked):
                out_ref[span * groups + group, own_chars + row : own_chars + row + 1, 0:verts] = value


def split_two(value):
    high = value.astype(jnp.bfloat16)
    return high, (value - high.astype(jnp.float32)).astype(jnp.bfloat16)


def across(lhs, rhs):
    return lax.dot_general(
        lhs, rhs, (((1,), (1,)), ((), ())), preferred_element_type=jnp.float32
    )


def shape_kernel(
    own_chars, groups, recv_ref, basis_ref, template_ref, regressor_ref, out_ref, basis_s, template_s, reg_s
):
    _, verts, block = basis_ref.shape
    joints = regressor_ref.shape[0]
    start = round_up(verts, SUBS)
    first = LANES - start
    rest = joints - first
    step = round_up(rest, SUBS)
    rows_in = recv_ref.shape[0]
    basis_s[...] = jnp.zeros_like(basis_s)
    for coord in range(3):
        basis_s[coord, 0:verts, 0:block] = basis_ref[coord]
    template_s[...] = jnp.zeros_like(template_s)
    template_s[0:3, 0:verts] = template_ref[...] * (1.0 / groups)
    reg_s[...] = jnp.zeros_like(reg_s)
    reg_s[start:LANES, 0:verts] = regressor_ref[0:first, :]
    reg_s[LANES : LANES + rest, 0:verts] = regressor_ref[first:joints, :]
    reg_high, reg_low = split_two(reg_s[...])
    reg_all = jnp.concatenate([reg_high, reg_low, reg_high], axis=1)
    per_source = recv_ref.shape[1]
    chunk = min(32, rows_in)

    def do_chunk(number):
        base = number * chunk
        coeffs = jnp.concatenate(
            [recv_ref[pl.ds(base, chunk), char, :] for char in range(own_chars)], axis=0
        ).astype(jnp.bfloat16)
        total = own_chars * chunk
        shapes = [
            across(coeffs, basis_s[coord]) + template_s[coord : coord + 1, :] for coord in range(3)
        ]
        stacked = jnp.concatenate(shapes, axis=0)
        high, low = split_two(stacked)
        sums = across(jnp.concatenate([high, high, low], axis=1), reg_all)
        last = jnp.zeros((total, LANES), jnp.float32)
        for coord in range(3):
            mine = sums[coord * total : (coord + 1) * total]
            extra = mine[:, LANES:]
            if coord:
                extra = pltpu.roll(extra, coord * step, 1)
            last = last + extra
            row = shapes[coord] + mine[:, :LANES]
            for char in range(own_chars):
                out_ref[pl.ds(base, chunk), 4 * char + coord, :] = row[char * chunk : (char + 1) * chunk]
        for char in range(own_chars):
            out_ref[pl.ds(base, chunk), 4 * char + 3, :] = last[char * chunk : (char + 1) * chunk]

    if rows_in == chunk:
        do_chunk(0)
    else:
        lax.fori_loop(0, rows_in // chunk, lambda number, carry: (do_chunk(number), carry)[1], 0)


def pick(table, index):
    return jnp.take_along_axis(table, index, axis=1, mode="promise_in_bounds")


def pose_kernel(
    groups, verts, skin_ref, recv_ref, quat_ref, shift_ref, parents_ref, out_ref, quat_s, parent_s, shift_s, sum_s, flat_s
):
    own_chars, _, joints = quat_ref.shape
    spans = recv_ref.shape[0] // groups
    half = SUBS // own_chars
    start = round_up(verts, SUBS)
    first = LANES - start
    step = round_up(joints - first, SUBS)
    lane = lax.broadcasted_iota(jnp.int32, (SUBS, LANES), 1)
    sub = lax.broadcasted_iota(jnp.int32, (SUBS, LANES), 0)

    def by_char(rows):
        value = jnp.broadcast_to(rows[0], (SUBS, LANES))
        for char in range(1, own_chars):
            value = jnp.where(sub >= char * half, rows[char], value)
        return value

    quat_s[...] = jnp.zeros_like(quat_s)
    quat_s[:, 0:1, :] = jnp.ones_like(quat_s[:, 0:1, :])
    quat_s[:, :, 0:joints] = quat_ref[...]
    quat = [by_char([quat_s[char, comp : comp + 1, :] for char in range(own_chars)]) for comp in range(4)]
    w, x, y, z = quat
    two = 2.0 / (w * w + x * x + y * y + z * z)
    rot = [
        [1.0 - two * (y * y + z * z), two * (x * y - w * z), two * (x * z + w * y)],
        [two * (x * y + w * z), 1.0 - two * (x * x + z * z), two * (y * z - w * x)],
        [two * (x * z - w * y), two * (y * z + w * x), 1.0 - two * (x * x + y * y)],
    ]
    parent_s[...] = jnp.zeros_like(parent_s)
    parent_s[0:1, 0:joints] = parents_ref[...]
    parent = jnp.broadcast_to(parent_s[0:1, :], (SUBS, LANES))
    above = jnp.where((lane >= joints) | (lane == 0), joints, parent)
    shift_s[...] = jnp.zeros_like(shift_s)
    shift_s[0:own_chars, 0:3] = shift_ref[...]
    shift = by_char([shift_s[char : char + 1, :] for char in range(own_chars)])

    total = None
    for span in range(spans):
        value = recv_ref[span * groups]
        for group in range(1, groups):
            value = value + recv_ref[span * groups + group]
        sum_s[span * SUBS : (span + 1) * SUBS, :] = value
        total = value if total is None else total + value
    places = []
    for coord in range(3):
        near = pltpu.roll(total, LANES - start, 1)
        far = pltpu.roll(total, (first - coord * step) % LANES, 1)
        near = by_char([near[4 * char + coord : 4 * char + coord + 1, :] for char in range(own_chars)])
        far = by_char([far[4 * char + 3 : 4 * char + 4, :] for char in range(own_chars)])
        places.append(jnp.where(lane < first, near, far))

    move = []
    for coord in range(3):
        origin = shift if coord == 0 else pltpu.roll(shift, LANES - coord, 1)
        offset = jnp.where(lane == 0, places[coord] + origin, places[coord] - pick(places[coord], parent))
        move.append(jnp.where(lane < joints, offset, 0.0))
    for level in range(max(1, (joints - 1).bit_length())):
        up = [[pick(rot[a][b], above) for b in range(3)] for a in range(3)]
        up_move = [pick(move[a], above) for a in range(3)]
        new_rot = [
            [up[a][0] * rot[0][b] + up[a][1] * rot[1][b] + up[a][2] * rot[2][b] for b in range(3)]
            for a in range(3)
        ]
        move = [
            up[a][0] * move[0] + up[a][1] * move[1] + up[a][2] * move[2] + up_move[a] for a in range(3)
        ]
        rot = new_rot
        above = pick(above, above)
    frames = [rot[a][b] for a in range(3) for b in range(3)]
    for a in range(3):
        frames.append(
            move[a] - (rot[a][0] * places[0] + rot[a][1] * places[1] + rot[a][2] * places[2])
        )

    slots = groups * ((skin_ref.shape[1] - own_chars) // 2)
    per_group = slots // groups
    for base in range(0, spans, SUBS):
        count = min(SUBS, spans - base)
        index, weight = [], []
        for slot in range(slots):
            group, which = slot // per_group, slot % per_group
            row = own_chars + 2 * which
            index.append(
                jnp.concatenate(
                    [skin_ref[(base + s) * groups + group, row : row + 1, :] for s in range(count)]
                    + [jnp.zeros((SUBS - count, LANES), jnp.float32)] * (count < SUBS),
                    axis=0,
                ).astype(jnp.int32)
            )
            weight.append(
                jnp.concatenate(
                    [skin_ref[(base + s) * groups + group, row + 1 : row + 2, :] for s in range(count)]
                    + [jnp.zeros((SUBS - count, LANES), jnp.float32)] * (count < SUBS),
                    axis=0,
                )
            )
        norm = functools.reduce(lambda p, q: p + q, weight)
        scale = 1.0 / jnp.where(norm > 0.0, norm, 1.0)
        weight = [value * scale for value in weight]
        for char in range(own_chars):
            blend = []
            for entry in range(12):
                table = jnp.broadcast_to(
                    frames[entry][char * half : char * half + 1, :], (SUBS, LANES)
                )
                value = weight[0] * pick(table, index[0])
                for slot in range(1, slots):
                    value = value + weight[slot] * pick(table, index[slot])
                blend.append(value)
            shaped = [
                jnp.concatenate(
                    [
                        sum_s[(base + s) * SUBS + 4 * char + coord : (base + s) * SUBS + 4 * char + coord + 1, :]
                        for s in range(count)
                    ]
                    + [jnp.zeros((SUBS - count, LANES), jnp.float32)] * (count < SUBS),
                    axis=0,
                )
                .astype(jnp.bfloat16)
                .astype(jnp.float32)
                for coord in range(3)
            ]
            for a in range(3):
                value = blend[9 + a]
                for m in range(3):
                    value = value + blend[3 * a + m] * shaped[m]
                for s in range(count):
                    low = (base + s) * verts
                    flat_s[a * own_chars + char : a * own_chars + char + 1, low : low + verts] = value[
                        s : s + 1, 0:verts
                    ]
    for a in range(3):
        out_ref[a] = flat_s[a * own_chars : (a + 1) * own_chars, :].astype(jnp.bfloat16)


def body(spans, groups, coeffs, shape_basis, template, regressor, quaternions, translation, parents, skin_index, skin_raw):
    own_chars, _ = coeffs.shape
    verts, slots = skin_index.shape
    joints = regressor.shape[0]
    devices = spans * groups
    rows = own_chars + 2 * slots // groups
    message = pl.pallas_call(
        functools.partial(pack_kernel, groups, spans, slots),
        out_shape=jax.ShapeDtypeStruct((devices, rows, LANES), jnp.float32),
        in_specs=[VMEM] * 3,
        out_specs=VMEM,
        name="pack",
    )(coeffs, skin_index.T, skin_raw.T)
    first_recv = lax.all_to_all(message, ("vert", "col"), 0, 0, tiled=True)
    partials = pl.pallas_call(
        functools.partial(shape_kernel, own_chars, groups),
        out_shape=jax.ShapeDtypeStruct((devices, 4 * own_chars, LANES), jnp.float32),
        in_specs=[VMEM] * 4,
        out_specs=VMEM,
        scratch_shapes=[
            pltpu.VMEM((3, LANES, LANES), jnp.bfloat16),
            pltpu.VMEM((SUBS, LANES), jnp.float32),
            pltpu.VMEM((2 * LANES, LANES), jnp.float32),
        ],
        name="shape",
    )(first_recv, shape_basis.transpose(1, 2, 0), template, regressor)
    second_recv = lax.all_to_all(partials, ("vert", "col"), 0, 0, tiled=True)
    posed = pl.pallas_call(
        functools.partial(pose_kernel, groups, verts),
        out_shape=jax.ShapeDtypeStruct((3, own_chars, spans * verts), jnp.bfloat16),
        in_specs=[VMEM] * 5,
        out_specs=VMEM,
        scratch_shapes=[
            pltpu.VMEM((own_chars, 4, LANES), jnp.float32),
            pltpu.VMEM((SUBS, LANES), jnp.int32),
            pltpu.VMEM((SUBS, LANES), jnp.float32),
            pltpu.VMEM((spans * SUBS, LANES), jnp.float32),
            pltpu.VMEM((SUBS, spans * verts), jnp.float32),
        ],
        name="pose",
    )(first_recv, second_recv, quaternions, translation, parents.reshape(1, joints))
    return posed.transpose(1, 0, 2)


def solution(mesh):
    in_specs = (
        P(("vert", "col"), None),
        P("col", None, "vert"),
        P(None, "vert"),
        P(None, "vert"),
        P(("vert", "col"), None, None),
        P(("vert", "col"), None),
        P(),
        P("vert", None),
        P("vert", None),
    )
    out_specs = P(("vert", "col"), None, None)
    return jax.shard_map(
        functools.partial(body, mesh.shape["vert"], mesh.shape["col"]),
        mesh=mesh,
        in_specs=in_specs,
        out_specs=out_specs,
        check_vma=False,
    )
```

```python
import functools

import jax
import jax.numpy as jnp
from jax import lax
from jax.experimental import pallas as pl
from jax.experimental.pallas import tpu as pltpu
from jax.sharding import PartitionSpec as P

LANES = 128
SUBS = 8
VMEM = pl.BlockSpec(memory_space=pltpu.VMEM)
HBM = pl.BlockSpec(memory_space=pltpu.HBM)
F32 = jnp.float32
BF16 = jnp.bfloat16


def round_up(value, step):
    return -(-value // step) * step


def layout(verts, joints):
    start = round_up(verts, SUBS)
    first = LANES - start
    rest = joints - first
    step = round_up(rest, SUBS)
    return start, first, rest, step


def in_hbm(*values):
    return [pltpu.with_memory_space_constraint(value, pltpu.HBM) for value in values]


def split_two(value):
    high = value.astype(BF16)
    return high, (value - high.astype(F32)).astype(BF16)


def dot(lhs, rhs):
    return jnp.dot(lhs, rhs, preferred_element_type=F32)


def each(count, limit, step):
    if count <= limit:
        for number in range(count):
            step(number)
    else:
        lax.fori_loop(0, count, lambda number, carry: (step(number), carry)[1], 0)


def dot_across(lhs, rhs):
    return lax.dot_general(lhs, rhs, (((1,), (1,)), ((), ())), preferred_element_type=F32)


def pick(table, index):
    return jnp.take_along_axis(table, index, axis=1, mode="promise_in_bounds")


def fetch(pairs, sems):
    copies = [pltpu.make_async_copy(src, dst, sems.at[n]) for n, (src, dst) in enumerate(pairs)]
    for copy in copies:
        copy.start()
    return copies


def pack_kernel(groups, spans, coeffs_hbm, index_hbm, raw_hbm, *refs):
    passed = (len(refs) - 5) // 2
    sources, out_ref, targets = refs[:passed], refs[passed], refs[passed + 1 : 2 * passed + 1]
    coeffs_s, index_s, raw_s, sems = refs[2 * passed + 1 :]
    copies = fetch(
        [(coeffs_hbm, coeffs_s), (index_hbm, index_s), (raw_hbm, raw_s), *zip(sources, targets)], sems
    )
    own_chars, comps = coeffs_s.shape
    block = comps // groups
    slots, verts = index_s.shape
    per_group = slots // groups
    column = lax.axis_index("col")
    out_ref[...] = jnp.zeros_like(out_ref)
    for copy in copies[:3]:
        copy.wait()
    wide = coeffs_s[...].astype(F32)
    index = index_s[...].astype(F32)
    raw = raw_s[...]
    picked = []
    for which in range(per_group):
        sel = lax.broadcasted_iota(jnp.int32, index.shape, 0) == column * per_group + which
        picked.append(jnp.sum(jnp.where(sel, index, 0.0), axis=0, keepdims=True))
        picked.append(jnp.sum(jnp.where(sel, raw, 0.0), axis=0, keepdims=True))
    for group in range(groups):
        piece = wide[:, group * block : (group + 1) * block]
        for span in range(spans):
            out_ref[span * groups + group, 0:own_chars, 0:block] = piece
            for row, value in enumerate(picked):
                at = own_chars + row
                out_ref[span * groups + group, at : at + 1, 0:verts] = value
    for copy in copies[3:]:
        copy.wait()


def shape_kernel(
    groups,
    recv_ref,
    basis_ref,
    template_ref,
    regressor_ref,
    quat_ref,
    move_ref,
    parents_ref,
    out_ref,
    diff_ref,
    shift_ref,
    coef_ref,
    weight_ref,
    pad_s,
    temp_s,
    reg_s,
    quat_s,
    parent_s,
    skin_s,
):
    _, verts, block = basis_ref.shape
    own_chars, _, joints = quat_ref.shape
    count = recv_ref.shape[0]
    spans = count // groups
    slots = skin_s.shape[0] // 2
    tiles = skin_s.shape[1] // LANES
    start, first, rest, step = layout(verts, joints)
    lane = lax.broadcasted_iota(jnp.int32, (SUBS, LANES), 1)
    sub = lax.broadcasted_iota(jnp.int32, (SUBS, LANES), 0)
    row = sub // own_chars

    pad_s[...] = jnp.zeros_like(pad_s)
    for coord in range(3):
        pad_s[coord, 0:verts, 0:block] = basis_ref[coord]
    temp_s[...] = jnp.zeros_like(temp_s)
    temp_s[0:3, 0:verts] = template_ref[...] * (1.0 / groups)
    reg_s[...] = jnp.zeros_like(reg_s)
    reg_s[start:LANES, 0:verts] = regressor_ref[0:first, :]
    reg_s[LANES : LANES + rest, 0:verts] = regressor_ref[first:joints, :]
    reg_high, reg_low = split_two(reg_s[...])
    reg_all = jnp.concatenate([reg_high, reg_low, reg_high], axis=1)
    chunk = min(32, count)
    total = own_chars * chunk

    def do_chunk(number):
        at = pl.ds(number * chunk, chunk)
        coeffs = jnp.concatenate([recv_ref[at, char, :] for char in range(own_chars)], axis=0).astype(BF16)
        shapes = [dot_across(coeffs, pad_s[coord]) + temp_s[coord : coord + 1, :] for coord in range(3)]
        high, low = split_two(jnp.concatenate(shapes, axis=0))
        sums = dot_across(jnp.concatenate([high, high, low], axis=1), reg_all)
        last = sums[0:total, LANES:]
        for coord in range(1, 3):
            last = last + pltpu.roll(sums[coord * total : (coord + 1) * total, LANES:], coord * step, 1)
        rows = [shapes[coord] + sums[coord * total : (coord + 1) * total, :LANES] for coord in range(3)]
        for place, value in enumerate(rows + [last]):
            for char in range(own_chars):
                out_ref[at, place * own_chars + char, :] = value[char * chunk : (char + 1) * chunk]

    each(count // chunk, 1, do_chunk)

    def by_char(rows):
        value = jnp.broadcast_to(rows[0], (SUBS, LANES))
        for char in range(1, own_chars):
            value = jnp.where(sub % own_chars == char, rows[char], value)
        return value

    quat_s[...] = jnp.zeros_like(quat_s)
    quat_s[:, 0:1, :] = jnp.ones_like(quat_s[:, 0:1, :])
    quat_s[:, :, 0:joints] = quat_ref[...]
    w, x, y, z = [
        by_char([quat_s[char, comp : comp + 1, :] for char in range(own_chars)]) for comp in range(4)
    ]
    two = 2.0 / (w * w + x * x + y * y + z * z)
    rot = [
        [1.0 - two * (y * y + z * z), two * (x * y - w * z), two * (x * z + w * y)],
        [two * (x * y + w * z), 1.0 - two * (x * x + z * z), two * (y * z - w * x)],
        [two * (x * z - w * y), two * (y * z + w * x), 1.0 - two * (x * x + y * y)],
    ]
    parent_s[...] = jnp.zeros_like(parent_s)
    parent_s[0:1, 0:joints] = parents_ref[...]
    parent = jnp.broadcast_to(parent_s[0:1, :], (SUBS, LANES))
    parent = jnp.where((lane >= joints) | (lane == 0), joints, parent)

    spot = lax.broadcasted_iota(jnp.int32, (LANES, LANES), 0)
    target = lax.broadcasted_iota(jnp.int32, (LANES, LANES), 1)
    inner = spot % step
    of_spot = jnp.where(
        spot >= start, spot - start, jnp.where((spot < 3 * step) & (inner < rest), first + inner, -1)
    )
    chain = jnp.where(of_spot == target, 1.0, 0.0)
    above = parent
    for _ in range(max(1, (joints - 1).bit_length())):
        up = [[pick(rot[a][b], above) for b in range(3)] for a in range(3)]
        rot = [
            [up[a][0] * rot[0][b] + up[a][1] * rot[1][b] + up[a][2] * rot[2][b] for b in range(3)]
            for a in range(3)
        ]
        chain = jnp.concatenate(
            [chain[n : n + SUBS] + pick(chain[n : n + SUBS], above) for n in range(0, LANES, SUBS)],
            axis=0,
        )
        above = pick(above, above)
    chain = chain.astype(BF16)

    tables = []
    for turn in range(3):
        value = rot[2][(2 + turn) % 3]
        for a in (1, 0):
            value = jnp.where(row == a, rot[a][(a + turn) % 3], value)
        tables.append(value)
    for a in range(3):
        value = jnp.zeros((SUBS, LANES), F32)
        for coord in range(3):
            diff = pick(rot[a][coord], parent) - rot[a][coord]
            near = pltpu.roll(diff, start, 1)
            far = pltpu.roll(diff, (coord * step - first) % LANES, 1)
            value = jnp.where((row == coord) & (lane >= start), near, value)
            value = jnp.where(
                (row == 3) & (lane >= coord * step) & (lane < coord * step + rest), far, value
            )
        diff_ref[a] = value
    moved = jnp.zeros((SUBS, LANES), F32)
    for char in range(own_chars):
        for a in range(3):
            moved = jnp.where(sub == a * own_chars + char, move_ref[char : char + 1, a : a + 1], moved)
    shift_ref[...] = moved

    skin_s[...] = jnp.zeros_like(skin_s)
    for span in range(spans):
        rows = jnp.concatenate(
            [recv_ref[span * groups + group, own_chars:, :] for group in range(groups)], axis=0
        )
        skin_s[:, span * verts : (span + 1) * verts] = rows[:, :verts]

    def do_tile(number, tables, chain):
        if isinstance(number, int):
            at = slice(number * LANES, (number + 1) * LANES)
        else:
            at = pl.ds(pl.multiple_of(number * LANES, LANES), LANES)
        skin = skin_s[:, at]
        index = [skin[2 * n : 2 * n + 1].astype(jnp.int32) for n in range(slots)]
        share = [skin[2 * n + 1 : 2 * n + 2] for n in range(slots)]
        norm = functools.reduce(lambda p, q: p + q, share)
        scale = 1.0 / jnp.where(norm > 0.0, norm, 1.0)
        share = [value * scale for value in share]
        wide = [jnp.broadcast_to(value, (SUBS, LANES)) for value in index]
        for turn in range(3):
            coef_ref[turn, :, at] = functools.reduce(
                lambda p, q: p + q, [share[n] * pick(tables[turn], wide[n]) for n in range(slots)]
            )
        grid = jnp.zeros((LANES, LANES), F32)
        for n in range(slots):
            grid = jnp.where(spot == index[n], share[n], grid)
        high, low = split_two(grid)
        closed = dot(chain, high) + dot(chain, low)
        high, low = split_two(closed)
        weight_ref[0:LANES, at] = high
        weight_ref[LANES : 2 * LANES, at] = low

    if tiles <= 8:
        for number in range(tiles):
            do_tile(number, tables, chain)
    else:
        carry = (tuple(tables), chain)
        lax.fori_loop(0, tiles, lambda number, kept: (do_tile(number, *kept), kept)[1], carry)


def pose_kernel(groups, own_chars, verts, recv_ref, diff_ref, shift_ref, coef_ref, weight_ref, out_ref):
    spans = recv_ref.shape[0] // groups
    width = out_ref.shape[2]
    tiles = coef_ref.shape[2] // LANES
    lane = lax.broadcasted_iota(jnp.int32, (SUBS, LANES), 1)
    sub = lax.broadcasted_iota(jnp.int32, (SUBS, LANES), 0)
    row = sub // own_chars
    total = None
    shapes = [None] * tiles
    for span in range(spans):
        value = recv_ref[span * groups]
        for group in range(1, groups):
            value = value + recv_ref[span * groups + group]
        total = value if total is None else total + value
        low = span * verts
        turned = pltpu.roll(value, low % LANES, 1) if low % LANES else value
        for tile in range(low // LANES, (low + verts - 1) // LANES + 1):
            begin = low - tile * LANES
            shapes[tile] = turned if begin <= 0 else jnp.where(lane >= begin, turned, shapes[tile])

    terms = []
    for a in range(3):
        term = diff_ref[a] * total
        step = own_chars
        while step < SUBS:
            term = term + pltpu.roll(term, step, 0)
            step *= 2
        terms.append(term)
    lhs = jnp.where(row == 0, terms[0], jnp.where(row == 1, terms[1], jnp.where(row == 2, terms[2], 0.0)))
    high = lhs.astype(BF16).astype(F32)
    left = jnp.concatenate([high, lhs - high], axis=0).astype(BF16)
    right = jnp.concatenate([high, jnp.zeros_like(high)], axis=0).astype(BF16)
    moved = dot(jnp.concatenate([left, right], axis=1), weight_ref[...])
    moved = moved[:SUBS] + moved[SUBS:]
    for tile in range(tiles):
        at = slice(tile * LANES, (tile + 1) * LANES)
        shape = shapes[tile].astype(BF16).astype(F32)
        by_one = pltpu.roll(shape, own_chars, 0)
        by_two = pltpu.roll(shape, 2 * own_chars, 0)
        by_three = pltpu.roll(shape, 3 * own_chars, 0)
        posed = (
            moved[:, at]
            + shift_ref[...]
            + coef_ref[0, :, at] * shape
            + coef_ref[1, :, at] * jnp.where(row < 2, by_three, by_two)
            + coef_ref[2, :, at] * jnp.where(row < 1, by_two, by_one)
        )
        end = min(width, (tile + 1) * LANES)
        for a in range(3):
            out_ref[a, :, tile * LANES : end] = posed[
                a * own_chars : (a + 1) * own_chars, : end - tile * LANES
            ].astype(BF16)


def body(spans, groups, coeffs, shape_basis, template, regressor, quaternions, translation, parents, skin_index, skin_raw):
    own_chars, comps = coeffs.shape
    verts, slots = skin_index.shape
    joints = regressor.shape[0]
    devices = spans * groups
    rows = own_chars + 2 * slots // groups
    padded = round_up(spans * verts, LANES)
    whole = jax.ShapeDtypeStruct
    room = pltpu.CompilerParams(vmem_limit_bytes=16 * 2**20)
    local = [
        shape_basis.transpose(1, 2, 0),
        template,
        regressor,
        quaternions,
        translation,
        parents.reshape(1, joints),
    ]
    message, *local = pl.pallas_call(
        functools.partial(pack_kernel, groups, spans),
        out_shape=[whole((devices, rows, LANES), F32)] + [whole(value.shape, value.dtype) for value in local],
        in_specs=[HBM] * (3 + len(local)),
        out_specs=[VMEM] * (1 + len(local)),
        scratch_shapes=[
            pltpu.VMEM((own_chars, comps), BF16),
            pltpu.VMEM((slots, verts), jnp.int32),
            pltpu.VMEM((slots, verts), F32),
            pltpu.SemaphoreType.DMA((3 + len(local),)),
        ],
        compiler_params=room,
        name="pack",
    )(*in_hbm(coeffs, skin_index.T, skin_raw.T, *local))
    received = lax.all_to_all(message, ("vert", "col"), 0, 0, tiled=True)
    partials, diff, shift, coef, weight = pl.pallas_call(
        functools.partial(shape_kernel, groups),
        out_shape=[
            whole((devices, 4 * own_chars, LANES), F32),
            whole((3, SUBS, LANES), F32),
            whole((SUBS, LANES), F32),
            whole((3, SUBS, padded), F32),
            whole((2 * LANES, padded), BF16),
        ],
        in_specs=[VMEM] * 7,
        out_specs=[VMEM] * 5,
        scratch_shapes=[
            pltpu.VMEM((3, LANES, LANES), BF16),
            pltpu.VMEM((SUBS, LANES), F32),
            pltpu.VMEM((2 * LANES, LANES), F32),
            pltpu.VMEM((own_chars, 4, LANES), F32),
            pltpu.VMEM((SUBS, LANES), jnp.int32),
            pltpu.VMEM((2 * slots, padded), F32),
        ],
        compiler_params=room,
        name="shape",
    )(received, *local)
    received = lax.all_to_all(partials, ("vert", "col"), 0, 0, tiled=True)
    posed = pl.pallas_call(
        functools.partial(pose_kernel, groups, own_chars, verts),
        out_shape=whole((3, own_chars, spans * verts), BF16),
        in_specs=[VMEM] * 5,
        out_specs=VMEM,
        compiler_params=room,
        name="pose",
    )(received, diff, shift, coef, weight)
    return posed.transpose(1, 0, 2)


def solution(mesh):
    in_specs = (
        P(("vert", "col"), None),
        P("col", None, "vert"),
        P(None, "vert"),
        P(None, "vert"),
        P(("vert", "col"), None, None),
        P(("vert", "col"), None),
        P(),
        P("vert", None),
        P("vert", None),
    )
    out_specs = P(("vert", "col"), None, None)
    return jax.shard_map(
        functools.partial(body, mesh.shape["vert"], mesh.shape["col"]),
        mesh=mesh,
        in_specs=in_specs,
        out_specs=out_specs,
        check_vma=False,
    )
```

```python
import functools
import math

import jax
import jax.numpy as jnp
from jax import lax
from jax.experimental import pallas as pl
from jax.experimental.pallas import tpu as pltpu
from jax.sharding import PartitionSpec as P

LANES = 128
SUBS = 8
VMEM = pl.BlockSpec(memory_space=pltpu.VMEM)
HBM = pl.BlockSpec(memory_space=pltpu.HBM)
F32 = jnp.float32
BF16 = jnp.bfloat16


def round_up(value, step):
    return -(-value // step) * step


def layout(verts, joints):
    start = round_up(verts, SUBS)
    first = LANES - start
    rest = joints - first
    step = round_up(rest, SUBS)
    return start, first, rest, step


def in_hbm(*values):
    return [pltpu.with_memory_space_constraint(value, pltpu.HBM) for value in values]


def split_two(value):
    high = value.astype(BF16)
    return high, (value - high.astype(F32)).astype(BF16)


def sum_of(values):
    return functools.reduce(lambda p, q: p + q, values)


def dot(lhs, rhs):
    return jnp.dot(lhs, rhs, preferred_element_type=F32)


def each(count, limit, step):
    if count <= limit:
        for number in range(count):
            step(number)
    else:
        lax.fori_loop(0, count, lambda number, carry: (step(number), carry)[1], 0)


def dot_across(lhs, rhs):
    return lax.dot_general(lhs, rhs, (((1,), (1,)), ((), ())), preferred_element_type=F32)


def pick(table, index):
    return jnp.take_along_axis(table, index, axis=1, mode="promise_in_bounds")


def fetch(pairs, sems):
    copies = [pltpu.make_async_copy(src, dst, sems.at[n]) for n, (src, dst) in enumerate(pairs)]
    for copy in copies:
        copy.start()
    return copies


def coder(verts, block):
    shape = block * 6.0 * 0.3125 + 6.0
    limit = max(shape, verts * 0.5 * shape)
    unit = 2.0**-16
    rate = math.log1p(limit / unit) / 32766.0
    return unit, rate


def pack_kernel(groups, spans, coeffs_hbm, index_hbm, raw_hbm, *refs):
    passed = (len(refs) - 6) // 2
    sources, out_ref, targets = refs[:passed], refs[passed], refs[passed + 1 : 2 * passed + 1]
    coeffs_s, index_s, raw_s, row_s, sems = refs[2 * passed + 1 :]
    copies = fetch(
        [(coeffs_hbm, coeffs_s), (index_hbm, index_s), (raw_hbm, raw_s), *zip(sources, targets)], sems
    )
    own_chars, comps = coeffs_s.shape
    block = comps // groups
    slots, verts = index_s.shape
    per_group = slots // groups
    column = lax.axis_index("col")
    row_s[...] = jnp.zeros_like(row_s)
    for copy in copies[:3]:
        copy.wait()
    wide = coeffs_s[...].astype(F32)
    index = index_s[...].astype(F32)
    raw = raw_s[...]
    for which in range(per_group):
        sel = lax.broadcasted_iota(jnp.int32, index.shape, 0) == column * per_group + which
        at = own_chars + 2 * which
        for more, value in enumerate((index, raw)):
            value = jnp.sum(jnp.where(sel, value, 0.0), axis=0, keepdims=True)
            for group in range(groups):
                row_s[group, at + more : at + more + 1, 0:verts] = value
    for group in range(groups):
        row_s[group, 0:own_chars, 0:block] = wide[:, group * block : (group + 1) * block]
    for group in range(groups):
        value = row_s[group]
        for span in range(spans):
            out_ref[span * groups + group] = value
    for copy in copies[3:]:
        copy.wait()


def shape_kernel(
    groups,
    recv_ref,
    basis_ref,
    template_ref,
    regressor_ref,
    quat_ref,
    move_ref,
    parents_ref,
    out_ref,
    table_ref,
    diff_ref,
    above_ref,
    shift_ref,
    index_ref,
    share_ref,
    pad_s,
    temp_s,
    reg_s,
    quat_s,
    parent_s,
    skin_s,
    sum_s,
):
    _, verts, block = basis_ref.shape
    own_chars, _, joints = quat_ref.shape
    count = recv_ref.shape[0]
    spans = count // groups
    slots = index_ref.shape[0]
    start, first, rest, step = layout(verts, joints)
    lane = lax.broadcasted_iota(jnp.int32, (SUBS, LANES), 1)
    sub = lax.broadcasted_iota(jnp.int32, (SUBS, LANES), 0)
    row = sub // own_chars
    char_of = sub % own_chars

    def by_char(rows):
        value = jnp.broadcast_to(rows[0], (SUBS, LANES))
        for char in range(1, own_chars):
            value = jnp.where(char_of == char, rows[char], value)
        return value

    def by_row(values):
        value = values[-1]
        for n in range(len(values) - 2, -1, -1):
            value = jnp.where(row == n, values[n], value)
        return value

    pad_s[...] = jnp.zeros_like(pad_s)
    for coord in range(3):
        pad_s[coord, 0:verts, 0:block] = basis_ref[coord]
    temp_s[...] = jnp.zeros_like(temp_s)
    temp_s[0:3, 0:verts] = template_ref[...] * (1.0 / groups)
    reg_s[...] = jnp.zeros_like(reg_s)
    reg_s[start:LANES, 0:verts] = regressor_ref[0:first, :]
    reg_s[LANES : LANES + rest, 0:verts] = regressor_ref[first:joints, :]
    reg_high, reg_low = split_two(reg_s[...])
    reg_all = jnp.concatenate([reg_high, reg_low, reg_high], axis=1)
    chunk = min(32, count)
    total = own_chars * chunk
    unit, rate = coder(verts, block)

    def do_chunk(number):
        at = pl.ds(number * chunk, chunk)
        coeffs = jnp.concatenate([recv_ref[at, char, :] for char in range(own_chars)], axis=0).astype(BF16)
        shapes = [dot_across(coeffs, pad_s[coord]) + temp_s[coord : coord + 1, :] for coord in range(3)]
        high, low = split_two(jnp.concatenate(shapes, axis=0))
        sums = dot_across(jnp.concatenate([high, high, low], axis=1), reg_all)
        last = sums[0:total, LANES:]
        for coord in range(1, 3):
            last = last + pltpu.roll(sums[coord * total : (coord + 1) * total, LANES:], coord * step, 1)
        rows = [shapes[coord] + sums[coord * total : (coord + 1) * total, :LANES] for coord in range(3)]
        for place, value in enumerate(rows + [last]):
            code = jnp.log(1.0 + jnp.abs(value) * (1.0 / unit)) * (1.0 / rate)
            code = jnp.where(value < 0.0, -code, code)
            for char in range(own_chars):
                sum_s[:, place * own_chars + char, :] = code[char * chunk : (char + 1) * chunk]
        out_ref[at] = jnp.round(sum_s[...]).astype(jnp.int32).astype(jnp.int16)

    each(count // chunk, 1, do_chunk)

    quat_s[...] = jnp.zeros_like(quat_s)
    quat_s[:, 0:1, :] = jnp.ones_like(quat_s[:, 0:1, :])
    quat_s[:, :, 0:joints] = quat_ref[...]
    w, x, y, z = [
        by_char([quat_s[char, comp : comp + 1, :] for char in range(own_chars)]) for comp in range(4)
    ]
    two = 2.0 / (w * w + x * x + y * y + z * z)
    rot = [
        by_row([1.0 - two * (y * y + z * z), two * (x * y + w * z), two * (x * z - w * y)]),
        by_row([two * (x * y - w * z), 1.0 - two * (x * x + z * z), two * (y * z + w * x)]),
        by_row([two * (x * z + w * y), two * (y * z - w * x), 1.0 - two * (x * x + y * y)]),
    ]
    parent_s[...] = jnp.zeros_like(parent_s)
    parent_s[0:1, 0:joints] = parents_ref[...]
    parent = jnp.broadcast_to(parent_s[0:1, :], (SUBS, LANES))
    parent = jnp.where((lane >= joints) | (lane == 0), joints, parent)

    wide = round_up(joints, SUBS)
    spot = lax.broadcasted_iota(jnp.int32, (wide, LANES), 0)
    target = lax.broadcasted_iota(jnp.int32, (wide, LANES), 1)
    chain = jnp.where((spot == target) & (target < joints), 1.0, 0.0)
    chain = [chain[n : n + SUBS] for n in range(0, wide, SUBS)]
    above = parent
    levels = max(1, (joints - 1).bit_length())
    for level in range(levels):
        spread = []
        for b in range(3):
            turned = [rot[b]] + [pltpu.roll(rot[b], n * own_chars, 0) for n in range(1, 4)]
            spread.append([by_row([turned[(r - m) % 4] for r in range(3)]) for m in range(3)])
        up = [pick(rot[b], above) for b in range(3)]
        rot = [sum_of([up[m] * spread[b][m] for m in range(3)]) for b in range(3)]
        chain = [value + pick(value, above) for value in chain]
        if level + 1 < levels:
            above = pick(above, above)

    for turn in range(3):
        table_ref[turn] = by_row([rot[(a + turn) % 3] for a in range(3)])
    far = jnp.zeros((SUBS, LANES), F32)
    for coord in range(3):
        diff = pick(rot[coord], parent) - rot[coord]
        diff_ref[coord] = jnp.where(lane >= start, pltpu.roll(diff, start, 1), 0.0)
        turned = pltpu.roll(diff, (coord * step - first) % LANES, 1)
        far = jnp.where((lane >= coord * step) & (lane < coord * step + rest), turned, far)
    diff_ref[3] = far
    none = jnp.zeros((SUBS, LANES), F32)
    tail = chain[first // SUBS :]
    tail = tail + [none] * (step // SUBS - len(tail))
    body = chain[: first // SUBS]
    middle = [none] * ((start - 3 * step) // SUBS)
    above_ref[...] = jnp.concatenate(tail * 3 + middle + body, axis=0).astype(BF16)
    moved = none
    for char in range(own_chars):
        for a in range(3):
            moved = jnp.where(sub == a * own_chars + char, move_ref[char : char + 1, a : a + 1], moved)
    shift_ref[...] = moved

    for span in range(spans):
        for group in range(groups):
            value = recv_ref[span * groups + group, own_chars:, :]
            rows = value.shape[0]
            skin_s[group * rows : (group + 1) * rows, span * verts : (span + 1) * verts] = value[:, :verts]
    norm = sum_of([skin_s[2 * n + 1 : 2 * n + 2, :] for n in range(slots)])
    scale = 1.0 / norm
    index_ref[...] = jnp.zeros_like(index_ref)
    share_ref[...] = jnp.zeros_like(share_ref)
    for n in range(slots):
        index_ref[n : n + 1, : spans * verts] = skin_s[2 * n : 2 * n + 1, :].astype(jnp.int32)
        share_ref[n : n + 1, : spans * verts] = skin_s[2 * n + 1 : 2 * n + 2, :] * scale


def pose_kernel(
    groups,
    own_chars,
    verts,
    block,
    recv_ref,
    table_ref,
    diff_ref,
    above_ref,
    shift_ref,
    index_ref,
    share_ref,
    out_ref,
    total_s,
):
    spans = recv_ref.shape[0] // groups
    slots = index_ref.shape[0]
    width = out_ref.shape[2]
    tiles = -(-width // LANES)
    lane = lax.broadcasted_iota(jnp.int32, (SUBS, LANES), 1)
    sub = lax.broadcasted_iota(jnp.int32, (SUBS, LANES), 0)
    row = sub // own_chars
    char_of = sub % own_chars
    unit, rate = coder(verts, block)

    def decode(number):
        code = recv_ref[number].astype(jnp.int32).astype(F32)
        value = jnp.exp(jnp.abs(code) * rate) * unit - unit
        return jnp.where(code < 0.0, -value, value)

    total = None
    shapes = [None] * tiles
    for span in range(spans):
        value = sum_of([decode(span * groups + group) for group in range(groups)])
        total = value if total is None else total + value
        low = span * verts
        turned = pltpu.roll(value, low % LANES, 1) if low % LANES else value
        for tile in range(low // LANES, (low + verts - 1) // LANES + 1):
            begin = low - tile * LANES
            shapes[tile] = turned if begin <= 0 else jnp.where(lane >= begin, turned, shapes[tile])

    total_s[...] = total
    terms = []
    for coord in range(4):
        pair = jnp.broadcast_to(total_s[coord * own_chars : coord * own_chars + 1, :], (SUBS, LANES))
        for char in range(1, own_chars):
            at = coord * own_chars + char
            pair = jnp.where(char_of == char, total_s[at : at + 1, :], pair)
        terms.append(diff_ref[coord] * pair)
    lhs = (terms[0] + terms[1]) + (terms[2] + terms[3])
    high = lhs.astype(BF16).astype(F32)
    moved = dot(jnp.concatenate([high, lhs - high], axis=0).astype(BF16), above_ref[...])
    moved = (moved[:SUBS] + moved[SUBS:]) + shift_ref[...]
    tables = [table_ref[turn] for turn in range(3)]
    for tile in range(tiles):
        end = min(width, (tile + 1) * LANES)
        at = slice(tile * LANES, (tile + 1) * LANES)
        index = [jnp.broadcast_to(index_ref[n : n + 1, at], (SUBS, LANES)) for n in range(slots)]
        share = [share_ref[n : n + 1, at] for n in range(slots)]

        def blend(table):
            return sum_of([share[n] * pick(table, index[n]) for n in range(slots)])

        shape = shapes[tile].astype(BF16).astype(F32)
        by_one = pltpu.roll(shape, own_chars, 0)
        by_two = pltpu.roll(shape, 2 * own_chars, 0)
        by_three = pltpu.roll(shape, 3 * own_chars, 0)
        turned = (
            blend(tables[0]) * shape
            + blend(tables[1]) * jnp.where(row < 2, by_three, by_two)
            + blend(tables[2]) * jnp.where(row < 1, by_two, by_one)
        )
        posed = turned + blend(moved)
        for a in range(3):
            out_ref[a, :, tile * LANES : end] = posed[
                a * own_chars : (a + 1) * own_chars, : end - tile * LANES
            ].astype(BF16)


def body(spans, groups, coeffs, shape_basis, template, regressor, quaternions, translation, parents, skin_index, skin_raw):
    own_chars, comps = coeffs.shape
    verts, slots = skin_index.shape
    joints = regressor.shape[0]
    devices = spans * groups
    block = comps // groups
    rows = own_chars + 2 * slots // groups
    padded = round_up(spans * verts, LANES)
    whole = jax.ShapeDtypeStruct
    room = pltpu.CompilerParams(vmem_limit_bytes=16 * 2**20)
    local = [
        shape_basis.transpose(1, 2, 0),
        template,
        regressor,
        quaternions,
        translation,
        parents.reshape(1, joints),
    ]
    message, *local = pl.pallas_call(
        functools.partial(pack_kernel, groups, spans),
        out_shape=[whole((devices, rows, LANES), F32)] + [whole(value.shape, value.dtype) for value in local],
        in_specs=[HBM] * (3 + len(local)),
        out_specs=[VMEM] * (1 + len(local)),
        scratch_shapes=[
            pltpu.VMEM((own_chars, comps), BF16),
            pltpu.VMEM((slots, verts), jnp.int32),
            pltpu.VMEM((slots, verts), F32),
            pltpu.VMEM((groups, rows, LANES), F32),
            pltpu.SemaphoreType.DMA((3 + len(local),)),
        ],
        compiler_params=room,
        name="pack",
    )(*in_hbm(coeffs, skin_index.T, skin_raw.T, *local))
    received = lax.all_to_all(message, ("vert", "col"), 0, 0, tiled=True)
    partials, *local = pl.pallas_call(
        functools.partial(shape_kernel, groups),
        out_shape=[
            whole((devices, 4 * own_chars, LANES), jnp.int16),
            whole((3, SUBS, LANES), F32),
            whole((4, SUBS, LANES), F32),
            whole((LANES, LANES), BF16),
            whole((SUBS, LANES), F32),
            whole((slots, padded), jnp.int32),
            whole((slots, padded), F32),
        ],
        in_specs=[VMEM] * 7,
        out_specs=[VMEM] * 7,
        scratch_shapes=[
            pltpu.VMEM((3, LANES, LANES), BF16),
            pltpu.VMEM((SUBS, LANES), F32),
            pltpu.VMEM((2 * LANES, LANES), F32),
            pltpu.VMEM((own_chars, 4, LANES), F32),
            pltpu.VMEM((SUBS, LANES), jnp.int32),
            pltpu.VMEM((2 * slots, spans * verts), F32),
            pltpu.VMEM((min(32, devices), 4 * own_chars, LANES), F32),
        ],
        compiler_params=room,
        name="shape",
    )(received, *local)
    received = lax.all_to_all(partials, ("vert", "col"), 0, 0, tiled=True)
    posed = pl.pallas_call(
        functools.partial(pose_kernel, groups, own_chars, verts, block),
        out_shape=whole((3, own_chars, spans * verts), BF16),
        in_specs=[VMEM] * 7,
        out_specs=VMEM,
        scratch_shapes=[pltpu.VMEM((SUBS, LANES), F32)],
        compiler_params=room,
        name="pose",
    )(received, *local)
    return posed.transpose(1, 0, 2)


def solution(mesh):
    in_specs = (
        P(("vert", "col"), None),
        P("col", None, "vert"),
        P(None, "vert"),
        P(None, "vert"),
        P(("vert", "col"), None, None),
        P(("vert", "col"), None),
        P(),
        P("vert", None),
        P("vert", None),
    )
    out_specs = P(("vert", "col"), None, None)
    return jax.shard_map(
        functools.partial(body, mesh.shape["vert"], mesh.shape["col"]),
        mesh=mesh,
        in_specs=in_specs,
        out_specs=out_specs,
        check_vma=False,
    )
```

```python
import functools
import math

import jax
import jax.numpy as jnp
from jax import lax
from jax.experimental import pallas as pl
from jax.experimental.pallas import tpu as pltpu
from jax.sharding import PartitionSpec as P

LANES = 128
SUBS = 8
VMEM = pl.BlockSpec(memory_space=pltpu.VMEM)
HBM = pl.BlockSpec(memory_space=pltpu.HBM)
F32 = jnp.float32
BF16 = jnp.bfloat16


def round_up(value, step):
    return -(-value // step) * step


def layout(verts, joints):
    start = round_up(verts, SUBS)
    first = LANES - start
    rest = joints - first
    step = round_up(rest, SUBS)
    return start, first, rest, step


def in_hbm(*values):
    return [pltpu.with_memory_space_constraint(value, pltpu.HBM) for value in values]


def split_two(value):
    high = value.astype(BF16)
    return high, (value - high.astype(F32)).astype(BF16)


def sum_of(values):
    return functools.reduce(lambda p, q: p + q, values)


def dot(lhs, rhs):
    return jnp.dot(lhs, rhs, preferred_element_type=F32)


def each(count, limit, step):
    if count <= limit:
        for number in range(count):
            step(number)
    else:
        lax.fori_loop(0, count, lambda number, carry: (step(number), carry)[1], 0)


def dot_across(lhs, rhs):
    return lax.dot_general(lhs, rhs, (((1,), (1,)), ((), ())), preferred_element_type=F32)


def pick(table, index):
    return jnp.take_along_axis(table, index, axis=1, mode="promise_in_bounds")


def fetch(pairs, sems):
    copies = [pltpu.make_async_copy(src, dst, sems.at[n]) for n, (src, dst) in enumerate(pairs)]
    for copy in copies:
        copy.start()
    return copies


def member(place, half):
    return (place + half - 1) % half


def halves(spans, groups, root):
    half = groups // 2
    return [
        [
            (root + span) % spans * groups + side * half + member(place, half)
            for span in range(spans)
            for place in range(half)
        ]
        for side in range(2)
    ]


def coder(verts, block):
    shape = block * 6.0 * 0.3125 + 6.0
    limit = max(shape, verts * 0.5 * shape)
    unit = 2.0**-16
    rate = math.log1p(limit / unit) / 32766.0
    return unit, rate


def pack_kernel(groups, spans, coeffs_hbm, index_hbm, raw_hbm, *refs):
    passed = (len(refs) - 6) // 2
    sources, out_ref, targets = refs[:passed], refs[passed], refs[passed + 1 : 2 * passed + 1]
    coeffs_s, index_s, raw_s, row_s, sems = refs[2 * passed + 1 :]
    copies = fetch(
        [(coeffs_hbm, coeffs_s), (index_hbm, index_s), (raw_hbm, raw_s), *zip(sources, targets)], sems
    )
    own_chars, comps = coeffs_s.shape
    half = groups // 2
    block = comps // groups
    slots, verts = index_s.shape
    per_group = slots // half
    column = lax.rem(lax.axis_index("col"), half)
    row_s[...] = jnp.zeros_like(row_s)
    for copy in copies[:3]:
        copy.wait()
    wide = coeffs_s[...].astype(F32)
    index = index_s[...].astype(F32)
    raw = raw_s[...]
    for which in range(per_group):
        sel = lax.broadcasted_iota(jnp.int32, index.shape, 0) == column * per_group + which
        at = 2 * own_chars + 2 * which
        for more, value in enumerate((index, raw)):
            value = jnp.sum(jnp.where(sel, value, 0.0), axis=0, keepdims=True)
            for place in range(half):
                row_s[place, at + more : at + more + 1, 0:verts] = value
    for place in range(half):
        for side in range(2):
            low = (side * half + member(place, half)) * block
            row_s[place, side * own_chars : (side + 1) * own_chars, 0:block] = wide[:, low : low + block]
    for place in range(half):
        value = row_s[place]
        for span in range(spans):
            out_ref[span * half + place] = value
    for copy in copies[3:]:
        copy.wait()


def shape_kernel(
    half,
    slots,
    root,
    turn,
    flat_ref,
    other_ref,
    basis_ref,
    template_ref,
    regressor_ref,
    quat_ref,
    move_ref,
    parents_ref,
    out_ref,
    table_ref,
    diff_ref,
    above_ref,
    shift_ref,
    index_ref,
    share_ref,
    pad_s,
    temp_s,
    reg_s,
    quat_s,
    parent_s,
    skin_s,
    sum_s,
):
    _, verts, block = basis_ref.shape
    own_chars, _, joints = quat_ref.shape
    height = 2 * own_chars + 2 * slots // half
    count = flat_ref.shape[0] // height
    spans = count // half
    start, first, rest, step = layout(verts, joints)
    lane = lax.broadcasted_iota(jnp.int32, (SUBS, LANES), 1)
    sub = lax.broadcasted_iota(jnp.int32, (SUBS, LANES), 0)
    row = sub // own_chars
    char_of = sub % own_chars

    def by_char(rows):
        value = jnp.broadcast_to(rows[0], (SUBS, LANES))
        for char in range(1, own_chars):
            value = jnp.where(char_of == char, rows[char], value)
        return value

    def by_row(values):
        value = values[-1]
        for n in range(len(values) - 2, -1, -1):
            value = jnp.where(row == n, values[n], value)
        return value

    side = lax.div(lax.axis_index("col"), half)
    pad_s[...] = jnp.zeros_like(pad_s)
    for coord in range(3):
        pad_s[side, coord, 0:verts, 0:block] = basis_ref[coord]
        pad_s[1 - side, coord, 0:verts, 0:block] = other_ref[coord]
    temp_s[...] = jnp.zeros_like(temp_s)
    temp_s[0:3, 0:verts] = template_ref[...] * (1.0 / half)
    reg_s[...] = jnp.zeros_like(reg_s)
    reg_s[start:LANES, 0:verts] = regressor_ref[0:first, :]
    reg_s[LANES : LANES + rest, 0:verts] = regressor_ref[first:joints, :]
    reg_high, reg_low = split_two(reg_s[...])
    reg_all = jnp.concatenate([reg_high, reg_low, reg_high], axis=1)
    chunk = min(16, count)
    total = own_chars * chunk
    unit, rate = coder(verts, 2 * block)

    def do_chunk(number):
        at = number * chunk * height
        coeffs = jnp.concatenate(
            [
                jnp.concatenate(
                    [
                        flat_ref[pl.ds(at + part * own_chars + char, chunk, stride=height), :]
                        for char in range(own_chars)
                    ],
                    axis=0,
                )
                for part in range(2)
            ],
            axis=1,
        ).astype(BF16)
        shapes = [
            dot_across(coeffs, jnp.concatenate([pad_s[0, coord], pad_s[1, coord]], axis=1))
            + temp_s[coord : coord + 1, :]
            for coord in range(3)
        ]
        high, low = split_two(jnp.concatenate(shapes, axis=0))
        sums = dot_across(jnp.concatenate([high, high, low], axis=1), reg_all)
        last = sums[0:total, LANES:]
        for coord in range(1, 3):
            last = last + pltpu.roll(sums[coord * total : (coord + 1) * total, LANES:], coord * step, 1)
        rows = [shapes[coord] + sums[coord * total : (coord + 1) * total, :LANES] for coord in range(3)]
        for place, value in enumerate(rows + [last]):
            code = jnp.log(1.0 + jnp.abs(value) * (1.0 / unit)) * (1.0 / rate)
            code = jnp.where(value < 0.0, -code, code)
            for char in range(own_chars):
                sum_s[pl.ds(number * chunk, chunk), place * own_chars + char, :] = code[
                    char * chunk : (char + 1) * chunk
                ]

    each(count // chunk, 1, do_chunk)
    for low, high, shift in ((0, count - turn, turn), (count - turn, count, turn - count)):
        out_ref[low + shift : high + shift] = jnp.round(sum_s[low:high]).astype(jnp.int32).astype(jnp.int16)

    quat_s[...] = jnp.zeros_like(quat_s)
    quat_s[:, 0:1, :] = jnp.ones_like(quat_s[:, 0:1, :])
    quat_s[:, :, 0:joints] = quat_ref[...]
    w, x, y, z = [
        by_char([quat_s[char, comp : comp + 1, :] for char in range(own_chars)]) for comp in range(4)
    ]
    two = 2.0 / (w * w + x * x + y * y + z * z)
    rot = [
        by_row([1.0 - two * (y * y + z * z), two * (x * y + w * z), two * (x * z - w * y)]),
        by_row([two * (x * y - w * z), 1.0 - two * (x * x + z * z), two * (y * z + w * x)]),
        by_row([two * (x * z + w * y), two * (y * z - w * x), 1.0 - two * (x * x + y * y)]),
    ]
    parent_s[...] = jnp.zeros_like(parent_s)
    parent_s[0:1, 0:joints] = parents_ref[...]
    parent = jnp.broadcast_to(parent_s[0:1, :], (SUBS, LANES))
    parent = jnp.where((lane >= joints) | (lane == 0), joints, parent)

    wide = round_up(joints, SUBS)
    spot = lax.broadcasted_iota(jnp.int32, (wide, LANES), 0)
    target = lax.broadcasted_iota(jnp.int32, (wide, LANES), 1)
    chain = jnp.where((spot == target) & (target < joints), 1.0, 0.0)
    chain = [chain[n : n + SUBS] for n in range(0, wide, SUBS)]
    above = parent
    levels = max(1, (joints - 1).bit_length())
    for level in range(levels):
        spread = []
        for b in range(3):
            turned = [rot[b]] + [pltpu.roll(rot[b], n * own_chars, 0) for n in range(1, 4)]
            spread.append([by_row([turned[(r - m) % 4] for r in range(3)]) for m in range(3)])
        up = [pick(rot[b], above) for b in range(3)]
        rot = [sum_of([up[m] * spread[b][m] for m in range(3)]) for b in range(3)]
        chain = [value + pick(value, above) for value in chain]
        if level + 1 < levels:
            above = pick(above, above)

    for turn in range(3):
        table_ref[turn] = by_row([rot[(a + turn) % 3] for a in range(3)])
    far = jnp.zeros((SUBS, LANES), F32)
    for coord in range(3):
        diff = pick(rot[coord], parent) - rot[coord]
        diff_ref[coord] = jnp.where(lane >= start, pltpu.roll(diff, start, 1), 0.0)
        turned = pltpu.roll(diff, (coord * step - first) % LANES, 1)
        far = jnp.where((lane >= coord * step) & (lane < coord * step + rest), turned, far)
    diff_ref[3] = far
    none = jnp.zeros((SUBS, LANES), F32)
    tail = chain[first // SUBS :]
    tail = tail + [none] * (step // SUBS - len(tail))
    body = chain[: first // SUBS]
    middle = [none] * ((start - 3 * step) // SUBS)
    above_ref[...] = jnp.concatenate(tail * 3 + middle + body, axis=0).astype(BF16)
    moved = none
    for char in range(own_chars):
        for a in range(3):
            moved = jnp.where(sub == a * own_chars + char, move_ref[char : char + 1, a : a + 1], moved)
    shift_ref[...] = moved

    per_group = slots // half
    for base in range(0, spans, SUBS):
        many = min(SUBS, spans - base)
        rows = [None] * (2 * slots)
        for place in range(half):
            for more in range(2 * per_group):
                at = (base * half + place) * height + 2 * own_chars + more
                rows[2 * per_group * member(place, half) + more] = flat_ref[
                    pl.ds(at, many, stride=half * height), :
                ]
        scale = 1.0 / sum_of(rows[1::2])
        rows[1::2] = [value * scale for value in rows[1::2]]
        for n, value in enumerate(rows):
            skin_s[pl.ds(base * 2 * slots + n, many, stride=2 * slots), :] = value
    tiles = index_ref.shape[1] // LANES
    values = [None] * tiles
    wide_lane = lax.broadcasted_iota(jnp.int32, (2 * slots, LANES), 1)
    for span in range(spans):
        at = (span - root) % spans * 2 * slots
        value = skin_s[at : at + 2 * slots, :]
        low = span * verts
        value = pltpu.roll(value, low % LANES, 1) if low % LANES else value
        for tile in range(low // LANES, (low + verts - 1) // LANES + 1):
            begin = low - tile * LANES
            values[tile] = value if begin <= 0 else jnp.where(wide_lane >= begin, value, values[tile])
    for tile in range(tiles):
        at = slice(tile * LANES, (tile + 1) * LANES)
        index_ref[:, at] = values[tile].astype(jnp.int32)
        share_ref[:, at] = values[tile]


def pose_kernel(
    half,
    root,
    own_chars,
    verts,
    block,
    recv_ref,
    table_ref,
    diff_ref,
    above_ref,
    shift_ref,
    index_ref,
    share_ref,
    out_ref,
    total_s,
):
    spans = recv_ref.shape[0] // half
    slots = index_ref.shape[0] // 2
    width = out_ref.shape[2]
    tiles = -(-width // LANES)
    lane = lax.broadcasted_iota(jnp.int32, (SUBS, LANES), 1)
    sub = lax.broadcasted_iota(jnp.int32, (SUBS, LANES), 0)
    row = sub // own_chars
    char_of = sub % own_chars
    unit, rate = coder(verts, 2 * block)

    def decode(number):
        code = recv_ref[number].astype(jnp.int32).astype(F32)
        value = jnp.exp(jnp.abs(code) * rate) * unit - unit
        return jnp.where(code < 0.0, -value, value)

    total = None
    shapes = [None] * tiles
    for span in range(spans):
        at = (span - root) % spans * half
        value = sum_of([decode(at + place) for place in range(half)])
        total = value if total is None else total + value
        low = span * verts
        turned = pltpu.roll(value, low % LANES, 1) if low % LANES else value
        for tile in range(low // LANES, (low + verts - 1) // LANES + 1):
            begin = low - tile * LANES
            shapes[tile] = turned if begin <= 0 else jnp.where(lane >= begin, turned, shapes[tile])

    total_s[...] = total
    terms = []
    for coord in range(4):
        pair = jnp.broadcast_to(total_s[coord * own_chars : coord * own_chars + 1, :], (SUBS, LANES))
        for char in range(1, own_chars):
            at = coord * own_chars + char
            pair = jnp.where(char_of == char, total_s[at : at + 1, :], pair)
        terms.append(diff_ref[coord] * pair)
    lhs = (terms[0] + terms[1]) + (terms[2] + terms[3])
    high = lhs.astype(BF16).astype(F32)
    moved = dot(jnp.concatenate([high, lhs - high], axis=0).astype(BF16), above_ref[...])
    moved = (moved[:SUBS] + moved[SUBS:]) + shift_ref[...]
    tables = [table_ref[turn] for turn in range(3)]
    for tile in range(tiles):
        end = min(width, (tile + 1) * LANES)
        at = slice(tile * LANES, (tile + 1) * LANES)
        index = [jnp.broadcast_to(index_ref[2 * n : 2 * n + 1, at], (SUBS, LANES)) for n in range(slots)]
        share = [share_ref[2 * n + 1 : 2 * n + 2, at] for n in range(slots)]

        def blend(table):
            return sum_of([share[n] * pick(table, index[n]) for n in range(slots)])

        shape = shapes[tile].astype(BF16).astype(F32)
        by_one = pltpu.roll(shape, own_chars, 0)
        by_two = pltpu.roll(shape, 2 * own_chars, 0)
        by_three = pltpu.roll(shape, 3 * own_chars, 0)
        turned = (
            blend(tables[0]) * shape
            + blend(tables[1]) * jnp.where(row < 2, by_three, by_two)
            + blend(tables[2]) * jnp.where(row < 1, by_two, by_one)
        )
        posed = turned + blend(moved)
        for a in range(3):
            out_ref[a, :, tile * LANES : end] = posed[
                a * own_chars : (a + 1) * own_chars, : end - tile * LANES
            ].astype(BF16)


def body(spans, groups, coeffs, shape_basis, template, regressor, quaternions, translation, parents, skin_index, skin_raw):
    own_chars, comps = coeffs.shape
    verts, slots = skin_index.shape
    joints = regressor.shape[0]
    half = groups // 2
    members = spans * half
    block = comps // groups
    rows = 2 * own_chars + 2 * slots // half
    roots = (spans // 2, spans // 4)
    turn = (roots[0] - roots[1]) % spans * half
    padded = round_up(spans * verts, LANES)
    whole = jax.ShapeDtypeStruct
    room = pltpu.CompilerParams(vmem_limit_bytes=16 * 2**20)
    local = [
        shape_basis.transpose(1, 2, 0),
        template,
        regressor,
        quaternions,
        translation,
        parents.reshape(1, joints),
    ]
    other = lax.ppermute(local[0], "col", [(n, (n + half) % groups) for n in range(groups)])

    def exchange(value, root):
        return lax.all_to_all(
            value, ("vert", "col"), 0, 0, tiled=True, axis_index_groups=halves(spans, groups, root)
        )

    message, *local = pl.pallas_call(
        functools.partial(pack_kernel, groups, spans),
        out_shape=[whole((members, rows, LANES), F32)] + [whole(value.shape, value.dtype) for value in local],
        in_specs=[HBM] * (3 + len(local)),
        out_specs=[VMEM] * (1 + len(local)),
        scratch_shapes=[
            pltpu.VMEM((own_chars, comps), BF16),
            pltpu.VMEM((slots, verts), jnp.int32),
            pltpu.VMEM((slots, verts), F32),
            pltpu.VMEM((half, rows, LANES), F32),
            pltpu.SemaphoreType.DMA((3 + len(local),)),
        ],
        compiler_params=room,
        name="pack",
    )(*in_hbm(coeffs, skin_index.T, skin_raw.T, *local))
    received = exchange(message, roots[0])
    partials, *local = pl.pallas_call(
        functools.partial(shape_kernel, half, slots, roots[0], turn),
        out_shape=[
            whole((members, 4 * own_chars, LANES), jnp.int16),
            whole((3, SUBS, LANES), F32),
            whole((4, SUBS, LANES), F32),
            whole((LANES, LANES), BF16),
            whole((SUBS, LANES), F32),
            whole((2 * slots, padded), jnp.int32),
            whole((2 * slots, padded), F32),
        ],
        in_specs=[VMEM] * 8,
        out_specs=[VMEM] * 7,
        scratch_shapes=[
            pltpu.VMEM((2, 3, LANES, LANES), BF16),
            pltpu.VMEM((SUBS, LANES), F32),
            pltpu.VMEM((2 * LANES, LANES), F32),
            pltpu.VMEM((own_chars, 4, LANES), F32),
            pltpu.VMEM((SUBS, LANES), jnp.int32),
            pltpu.VMEM((spans * 2 * slots, LANES), F32),
            pltpu.VMEM((members, 4 * own_chars, LANES), F32),
        ],
        compiler_params=room,
        name="shape",
    )(received.reshape(members * rows, LANES), other, *local)
    received = exchange(partials, roots[1])
    posed = pl.pallas_call(
        functools.partial(pose_kernel, half, roots[1], own_chars, verts, block),
        out_shape=whole((3, own_chars, spans * verts), BF16),
        in_specs=[VMEM] * 7,
        out_specs=VMEM,
        scratch_shapes=[pltpu.VMEM((SUBS, LANES), F32)],
        compiler_params=room,
        name="pose",
    )(received, *local)
    return posed.transpose(1, 0, 2)


def solution(mesh):
    in_specs = (
        P(("vert", "col"), None),
        P("col", None, "vert"),
        P(None, "vert"),
        P(None, "vert"),
        P(("vert", "col"), None, None),
        P(("vert", "col"), None),
        P(),
        P("vert", None),
        P("vert", None),
    )
    out_specs = P(("vert", "col"), None, None)
    return jax.shard_map(
        functools.partial(body, mesh.shape["vert"], mesh.shape["col"]),
        mesh=mesh,
        in_specs=in_specs,
        out_specs=out_specs,
        check_vma=False,
    )
```

```python
import functools
import math

import jax
import jax.numpy as jnp
from jax import lax
from jax.experimental import pallas as pl
from jax.experimental.pallas import tpu as pltpu
from jax.sharding import PartitionSpec as P

LANES = 128
SUBS = 8
VMEM = pl.BlockSpec(memory_space=pltpu.VMEM)
HBM = pl.BlockSpec(memory_space=pltpu.HBM)
F32 = jnp.float32
BF16 = jnp.bfloat16


def round_up(value, step):
    return -(-value // step) * step


def layout(verts, joints):
    start = round_up(verts, SUBS)
    first = LANES - start
    rest = joints - first
    step = round_up(rest, SUBS)
    return start, first, rest, step


def in_hbm(*values):
    return [pltpu.with_memory_space_constraint(value, pltpu.HBM) for value in values]


def split_two(value):
    high = value.astype(BF16)
    return high, (value - high.astype(F32)).astype(BF16)


def sum_of(values):
    return functools.reduce(lambda p, q: p + q, values)


def dot(lhs, rhs):
    return jnp.dot(lhs, rhs, preferred_element_type=F32)


def each(count, limit, step):
    if count <= limit:
        for number in range(count):
            step(number)
    else:
        lax.fori_loop(0, count, lambda number, carry: (step(number), carry)[1], 0)


def dot_across(lhs, rhs):
    return lax.dot_general(lhs, rhs, (((1,), (1,)), ((), ())), preferred_element_type=F32)


def pick(table, index):
    return jnp.take_along_axis(table, index, axis=1, mode="promise_in_bounds")


def fetch(pairs, sems):
    copies = [pltpu.make_async_copy(src, dst, sems.at[n]) for n, (src, dst) in enumerate(pairs)]
    for copy in copies:
        copy.start()
    return copies


def member(place, half):
    return (place + half - 1) % half


def halves(spans, groups, root):
    half = groups // 2
    return [
        [
            (root + span) % spans * groups + side * half + member(place, half)
            for span in range(spans)
            for place in range(half)
        ]
        for side in range(2)
    ]


def coder(verts, block):
    shape = block * 6.0 * 0.3125 + 6.0
    limit = max(shape, verts * 0.5 * shape)
    unit = 2.0**-16
    rate = math.log1p(limit / unit) / 32766.0
    return unit, rate


def pack_kernel(groups, spans, coeffs_hbm, index_hbm, raw_hbm, out_ref, coeffs_s, index_s, raw_s, row_s, sems):
    copies = fetch([(coeffs_hbm, coeffs_s), (index_hbm, index_s), (raw_hbm, raw_s)], sems)
    own_chars, comps = coeffs_s.shape
    half = groups // 2
    block = comps // groups
    slots, verts = index_s.shape
    per_group = slots // half
    column = lax.rem(lax.axis_index("col"), half)
    side = lax.div(lax.axis_index("col"), half)
    row_s[...] = jnp.zeros_like(row_s)
    for copy in copies:
        copy.wait()
    wide = coeffs_s[...].astype(F32)
    index = index_s[...].astype(F32)
    raw = raw_s[...]
    for which in range(per_group):
        sel = lax.broadcasted_iota(jnp.int32, index.shape, 0) == column * per_group + which
        at = 2 * own_chars + 2 * which
        for more, value in enumerate((index, raw)):
            value = jnp.sum(jnp.where(sel, value, 0.0), axis=0, keepdims=True)
            for place in range(half):
                row_s[place, at + more : at + more + 1, 0:verts] = value
    for place in range(half):
        low = [(part * half + member(place, half)) * block for part in range(2)]
        low = [wide[:, at : at + block] for at in low]
        row_s[place, 0:own_chars, 0:block] = jnp.where(side == 0, low[0], low[1])
        row_s[place, own_chars : 2 * own_chars, 0:block] = jnp.where(side == 0, low[1], low[0])
    for place in range(half):
        value = row_s[place]
        for span in range(spans):
            out_ref[span * half + place] = value


def prep_kernel(
    half,
    basis_hbm,
    template_hbm,
    regressor_hbm,
    quat_hbm,
    move_hbm,
    parents_hbm,
    own_ref,
    temp_ref,
    reg_ref,
    table_ref,
    diff_ref,
    above_ref,
    shift_ref,
    basis_s,
    template_s,
    regressor_s,
    quat_raw,
    move_s,
    parents_s,
    reg_s,
    quat_s,
    parent_s,
    sems,
):
    copies = fetch(
        [
            (basis_hbm, basis_s),
            (template_hbm, template_s),
            (regressor_hbm, regressor_s),
            (quat_hbm, quat_raw),
            (move_hbm, move_s),
            (parents_hbm, parents_s),
        ],
        sems,
    )
    _, verts, block = basis_s.shape
    own_chars, _, joints = quat_raw.shape
    start, first, rest, step = layout(verts, joints)
    lane = lax.broadcasted_iota(jnp.int32, (SUBS, LANES), 1)
    sub = lax.broadcasted_iota(jnp.int32, (SUBS, LANES), 0)
    row = sub // own_chars
    char_of = sub % own_chars

    def by_char(rows):
        value = jnp.broadcast_to(rows[0], (SUBS, LANES))
        for char in range(1, own_chars):
            value = jnp.where(char_of == char, rows[char], value)
        return value

    def by_row(values):
        value = values[-1]
        for n in range(len(values) - 2, -1, -1):
            value = jnp.where(row == n, values[n], value)
        return value

    own_ref[...] = jnp.zeros_like(own_ref)
    temp_ref[...] = jnp.zeros_like(temp_ref)
    reg_s[...] = jnp.zeros_like(reg_s)
    quat_s[...] = jnp.zeros_like(quat_s)
    quat_s[:, 0:1, :] = jnp.ones_like(quat_s[:, 0:1, :])
    parent_s[...] = jnp.zeros_like(parent_s)
    for copy in copies:
        copy.wait()
    for coord in range(3):
        own_ref[coord, 0:verts, 0:block] = basis_s[coord]
    temp_ref[0:3, 0:verts] = template_s[...] * (1.0 / half)
    reg_s[start:LANES, 0:verts] = regressor_s[0:first, :]
    reg_s[LANES : LANES + rest, 0:verts] = regressor_s[first:joints, :]
    high, low = split_two(reg_s[...])
    for n, value in enumerate((high, low, high)):
        reg_ref[:, n * LANES : (n + 1) * LANES] = value

    quat_s[:, :, 0:joints] = quat_raw[...]
    w, x, y, z = [
        by_char([quat_s[char, comp : comp + 1, :] for char in range(own_chars)]) for comp in range(4)
    ]
    two = 2.0 / (w * w + x * x + y * y + z * z)
    rot = [
        by_row([1.0 - two * (y * y + z * z), two * (x * y + w * z), two * (x * z - w * y)]),
        by_row([two * (x * y - w * z), 1.0 - two * (x * x + z * z), two * (y * z + w * x)]),
        by_row([two * (x * z + w * y), two * (y * z - w * x), 1.0 - two * (x * x + y * y)]),
    ]
    parent_s[0:1, 0:joints] = parents_s[...]
    parent = jnp.broadcast_to(parent_s[0:1, :], (SUBS, LANES))
    parent = jnp.where((lane >= joints) | (lane == 0), joints, parent)

    wide = round_up(joints, SUBS)
    spot = lax.broadcasted_iota(jnp.int32, (wide, LANES), 0)
    target = lax.broadcasted_iota(jnp.int32, (wide, LANES), 1)
    chain = jnp.where((spot == target) & (target < joints), 1.0, 0.0)
    chain = [chain[n : n + SUBS] for n in range(0, wide, SUBS)]
    above = parent
    levels = max(1, (joints - 1).bit_length())
    for level in range(levels):
        spread = []
        for b in range(3):
            turned = [rot[b]] + [pltpu.roll(rot[b], n * own_chars, 0) for n in range(1, 4)]
            spread.append([by_row([turned[(r - m) % 4] for r in range(3)]) for m in range(3)])
        up = [pick(rot[b], above) for b in range(3)]
        rot = [sum_of([up[m] * spread[b][m] for m in range(3)]) for b in range(3)]
        chain = [value + pick(value, above) for value in chain]
        if level + 1 < levels:
            above = pick(above, above)

    for turn in range(3):
        table_ref[turn] = by_row([rot[(a + turn) % 3] for a in range(3)])
    far = jnp.zeros((SUBS, LANES), F32)
    for coord in range(3):
        diff = pick(rot[coord], parent) - rot[coord]
        diff_ref[coord] = jnp.where(lane >= start, pltpu.roll(diff, start, 1), 0.0)
        turned = pltpu.roll(diff, (coord * step - first) % LANES, 1)
        far = jnp.where((lane >= coord * step) & (lane < coord * step + rest), turned, far)
    diff_ref[3] = far
    none = jnp.zeros((SUBS, LANES), F32)
    tail = chain[first // SUBS :]
    tail = tail + [none] * (step // SUBS - len(tail))
    body = chain[: first // SUBS]
    middle = [none] * ((start - 3 * step) // SUBS)
    above_ref[...] = jnp.concatenate(tail * 3 + middle + body, axis=0).astype(BF16)
    moved = none
    for char in range(own_chars):
        for a in range(3):
            moved = jnp.where(sub == a * own_chars + char, move_s[char : char + 1, a : a + 1], moved)
    shift_ref[...] = moved


def shape_kernel(
    half,
    own_chars,
    verts,
    slots,
    joints,
    root,
    turn,
    flat_ref,
    other_ref,
    own_ref,
    temp_ref,
    reg_ref,
    out_ref,
    index_ref,
    share_ref,
    pad_s,
    skin_s,
    sum_s,
):
    block = other_ref.shape[2]
    height = 2 * own_chars + 2 * slots // half
    count = flat_ref.shape[0] // height
    spans = count // half
    step = layout(verts, joints)[3]

    pad_s[...] = jnp.zeros_like(pad_s)
    for coord in range(3):
        pad_s[coord, 0:verts, 0:block] = other_ref[coord]
    chunk = min(16, count)
    total = own_chars * chunk
    unit, rate = coder(verts, 2 * block)

    def do_chunk(number):
        at = number * chunk * height
        coeffs = jnp.concatenate(
            [
                jnp.concatenate(
                    [
                        flat_ref[pl.ds(at + part * own_chars + char, chunk, stride=height), :]
                        for char in range(own_chars)
                    ],
                    axis=0,
                )
                for part in range(2)
            ],
            axis=1,
        ).astype(BF16)
        shapes = [
            dot_across(coeffs, jnp.concatenate([own_ref[coord], pad_s[coord]], axis=1))
            + temp_ref[coord : coord + 1, :]
            for coord in range(3)
        ]
        high, low = split_two(jnp.concatenate(shapes, axis=0))
        sums = dot_across(jnp.concatenate([high, high, low], axis=1), reg_ref[...])
        last = sums[0:total, LANES:]
        for coord in range(1, 3):
            last = last + pltpu.roll(sums[coord * total : (coord + 1) * total, LANES:], coord * step, 1)
        rows = [shapes[coord] + sums[coord * total : (coord + 1) * total, :LANES] for coord in range(3)]
        for place, value in enumerate(rows + [last]):
            code = jnp.log(1.0 + jnp.abs(value) * (1.0 / unit)) * (1.0 / rate)
            code = jnp.where(value < 0.0, -code, code)
            for char in range(own_chars):
                sum_s[pl.ds(number * chunk, chunk), place * own_chars + char, :] = code[
                    char * chunk : (char + 1) * chunk
                ]

    each(count // chunk, 1, do_chunk)
    for low, high, shift in ((0, count - turn, turn), (count - turn, count, turn - count)):
        if high > low:
            out_ref[low + shift : high + shift] = (
                jnp.round(sum_s[low:high]).astype(jnp.int32).astype(jnp.int16)
            )

    per_group = slots // half
    for base in range(0, spans, SUBS):
        many = min(SUBS, spans - base)
        rows = [None] * (2 * slots)
        for place in range(half):
            for more in range(2 * per_group):
                at = (base * half + place) * height + 2 * own_chars + more
                rows[2 * per_group * member(place, half) + more] = flat_ref[
                    pl.ds(at, many, stride=half * height), :
                ]
        scale = 1.0 / sum_of(rows[1::2])
        rows[1::2] = [value * scale for value in rows[1::2]]
        for n, value in enumerate(rows):
            skin_s[pl.ds(base * 2 * slots + n, many, stride=2 * slots), :] = value
    tiles = index_ref.shape[1] // LANES
    values = [None] * tiles
    wide_lane = lax.broadcasted_iota(jnp.int32, (2 * slots, LANES), 1)
    for span in range(spans):
        at = (span - root) % spans * 2 * slots
        value = skin_s[at : at + 2 * slots, :]
        low = span * verts
        value = pltpu.roll(value, low % LANES, 1) if low % LANES else value
        for tile in range(low // LANES, (low + verts - 1) // LANES + 1):
            begin = low - tile * LANES
            values[tile] = value if begin <= 0 else jnp.where(wide_lane >= begin, value, values[tile])
    for tile in range(tiles):
        at = slice(tile * LANES, (tile + 1) * LANES)
        index_ref[:, at] = values[tile].astype(jnp.int32)
        share_ref[:, at] = values[tile]


def pose_kernel(
    half,
    root,
    own_chars,
    verts,
    block,
    recv_ref,
    table_ref,
    diff_ref,
    above_ref,
    shift_ref,
    index_ref,
    share_ref,
    out_ref,
    total_s,
):
    spans = recv_ref.shape[0] // half
    slots = index_ref.shape[0] // 2
    width = out_ref.shape[2]
    tiles = -(-width // LANES)
    lane = lax.broadcasted_iota(jnp.int32, (SUBS, LANES), 1)
    sub = lax.broadcasted_iota(jnp.int32, (SUBS, LANES), 0)
    row = sub // own_chars
    char_of = sub % own_chars
    unit, rate = coder(verts, 2 * block)

    def decode(number):
        code = recv_ref[number].astype(jnp.int32).astype(F32)
        value = jnp.exp(jnp.abs(code) * rate) * unit - unit
        return jnp.where(code < 0.0, -value, value)

    total = None
    shapes = [None] * tiles
    for span in range(spans):
        at = (span - root) % spans * half
        value = sum_of([decode(at + place) for place in range(half)])
        total = value if total is None else total + value
        low = span * verts
        turned = pltpu.roll(value, low % LANES, 1) if low % LANES else value
        for tile in range(low // LANES, (low + verts - 1) // LANES + 1):
            begin = low - tile * LANES
            shapes[tile] = turned if begin <= 0 else jnp.where(lane >= begin, turned, shapes[tile])

    total_s[...] = total
    terms = []
    for coord in range(4):
        pair = jnp.broadcast_to(total_s[coord * own_chars : coord * own_chars + 1, :], (SUBS, LANES))
        for char in range(1, own_chars):
            at = coord * own_chars + char
            pair = jnp.where(char_of == char, total_s[at : at + 1, :], pair)
        terms.append(diff_ref[coord] * pair)
    lhs = (terms[0] + terms[1]) + (terms[2] + terms[3])
    high = lhs.astype(BF16).astype(F32)
    moved = dot(jnp.concatenate([high, lhs - high], axis=0).astype(BF16), above_ref[...])
    moved = (moved[:SUBS] + moved[SUBS:]) + shift_ref[...]
    tables = [table_ref[turn] for turn in range(3)]
    for tile in range(tiles):
        end = min(width, (tile + 1) * LANES)
        at = slice(tile * LANES, (tile + 1) * LANES)
        index = [jnp.broadcast_to(index_ref[2 * n : 2 * n + 1, at], (SUBS, LANES)) for n in range(slots)]
        share = [share_ref[2 * n + 1 : 2 * n + 2, at] for n in range(slots)]

        def blend(table):
            return sum_of([share[n] * pick(table, index[n]) for n in range(slots)])

        shape = shapes[tile].astype(BF16).astype(F32)
        by_one = pltpu.roll(shape, own_chars, 0)
        by_two = pltpu.roll(shape, 2 * own_chars, 0)
        by_three = pltpu.roll(shape, 3 * own_chars, 0)
        turned = (
            blend(tables[0]) * shape
            + blend(tables[1]) * jnp.where(row < 2, by_three, by_two)
            + blend(tables[2]) * jnp.where(row < 1, by_two, by_one)
        )
        posed = turned + blend(moved)
        for a in range(3):
            out_ref[a, :, tile * LANES : end] = posed[
                a * own_chars : (a + 1) * own_chars, : end - tile * LANES
            ].astype(BF16)


def body(spans, groups, coeffs, shape_basis, template, regressor, quaternions, translation, parents, skin_index, skin_raw):
    own_chars, comps = coeffs.shape
    verts, slots = skin_index.shape
    joints = regressor.shape[0]
    half = groups // 2
    members = spans * half
    block = comps // groups
    rows = 2 * own_chars + 2 * slots // half
    roots = (spans // 2, spans // 4)
    turn = (roots[0] - roots[1]) % spans * half
    padded = round_up(spans * verts, LANES)
    whole = jax.ShapeDtypeStruct
    room = pltpu.CompilerParams(vmem_limit_bytes=16 * 2**20)
    basis = shape_basis.transpose(1, 2, 0)
    other = lax.ppermute(basis, "col", [(n, (n + half) % groups) for n in range(groups)])

    def exchange(value, root):
        return lax.all_to_all(
            value, ("vert", "col"), 0, 0, tiled=True, axis_index_groups=halves(spans, groups, root)
        )

    message = pl.pallas_call(
        functools.partial(pack_kernel, groups, spans),
        out_shape=whole((members, rows, LANES), F32),
        in_specs=[HBM] * 3,
        out_specs=VMEM,
        scratch_shapes=[
            pltpu.VMEM((own_chars, comps), BF16),
            pltpu.VMEM((slots, verts), jnp.int32),
            pltpu.VMEM((slots, verts), F32),
            pltpu.VMEM((half, rows, LANES), F32),
            pltpu.SemaphoreType.DMA((3,)),
        ],
        compiler_params=room,
        name="pack",
    )(*in_hbm(coeffs, skin_index.T, skin_raw.T))
    received = exchange(message, roots[0])
    own, temp, reg, *local = pl.pallas_call(
        functools.partial(prep_kernel, half),
        out_shape=[
            whole((3, LANES, LANES), BF16),
            whole((SUBS, LANES), F32),
            whole((2 * LANES, 3 * LANES), BF16),
            whole((3, SUBS, LANES), F32),
            whole((4, SUBS, LANES), F32),
            whole((LANES, LANES), BF16),
            whole((SUBS, LANES), F32),
        ],
        in_specs=[HBM] * 6,
        out_specs=[VMEM] * 7,
        scratch_shapes=[
            pltpu.VMEM((3, verts, block), BF16),
            pltpu.VMEM((3, verts), F32),
            pltpu.VMEM((joints, verts), F32),
            pltpu.VMEM((own_chars, 4, joints), F32),
            pltpu.VMEM((own_chars, 3), F32),
            pltpu.VMEM((1, joints), jnp.int32),
            pltpu.VMEM((2 * LANES, LANES), F32),
            pltpu.VMEM((own_chars, 4, LANES), F32),
            pltpu.VMEM((SUBS, LANES), jnp.int32),
            pltpu.SemaphoreType.DMA((6,)),
        ],
        compiler_params=room,
        cost_estimate=pl.CostEstimate(flops=10**7, bytes_accessed=10**6, transcendentals=0),
        name="prep",
    )(*in_hbm(basis, template, regressor, quaternions, translation, parents.reshape(1, joints)))
    partials, *skin = pl.pallas_call(
        functools.partial(shape_kernel, half, own_chars, verts, slots, joints, roots[0], turn),
        out_shape=[
            whole((members, 4 * own_chars, LANES), jnp.int16),
            whole((2 * slots, padded), jnp.int32),
            whole((2 * slots, padded), F32),
        ],
        in_specs=[VMEM] * 5,
        out_specs=[VMEM] * 3,
        scratch_shapes=[
            pltpu.VMEM((3, LANES, LANES), BF16),
            pltpu.VMEM((spans * 2 * slots, LANES), F32),
            pltpu.VMEM((members, 4 * own_chars, LANES), F32),
        ],
        compiler_params=room,
        name="shape",
    )(received.reshape(members * rows, LANES), other, own, temp, reg)
    received = exchange(partials, roots[1])
    posed = pl.pallas_call(
        functools.partial(pose_kernel, half, roots[1], own_chars, verts, block),
        out_shape=whole((3, own_chars, spans * verts), BF16),
        in_specs=[VMEM] * 7,
        out_specs=VMEM,
        scratch_shapes=[pltpu.VMEM((SUBS, LANES), F32)],
        compiler_params=room,
        name="pose",
    )(received, *local, *skin)
    return posed.transpose(1, 0, 2)


def solution(mesh):
    in_specs = (
        P(("vert", "col"), None),
        P("col", None, "vert"),
        P(None, "vert"),
        P(None, "vert"),
        P(("vert", "col"), None, None),
        P(("vert", "col"), None),
        P(),
        P("vert", None),
        P("vert", None),
    )
    out_specs = P(("vert", "col"), None, None)
    return jax.shard_map(
        functools.partial(body, mesh.shape["vert"], mesh.shape["col"]),
        mesh=mesh,
        in_specs=in_specs,
        out_specs=out_specs,
        check_vma=False,
    )
```

```python
import functools
import math

import jax
import jax.numpy as jnp
from jax import lax
from jax.experimental import pallas as pl
from jax.experimental.pallas import tpu as pltpu
from jax.sharding import PartitionSpec as P

LANES = 128
SUBS = 8
VMEM = pl.BlockSpec(memory_space=pltpu.VMEM)
HBM = pl.BlockSpec(memory_space=pltpu.HBM)
F32 = jnp.float32
BF16 = jnp.bfloat16


def round_up(value, step):
    return -(-value // step) * step


def layout(verts, joints):
    start = round_up(verts, SUBS)
    first = LANES - start
    rest = joints - first
    step = round_up(rest, SUBS)
    return start, first, rest, step


def in_hbm(*values):
    return [pltpu.with_memory_space_constraint(value, pltpu.HBM) for value in values]


def split_two(value):
    high = value.astype(BF16)
    return high, (value - high.astype(F32)).astype(BF16)


def sum_of(values):
    return functools.reduce(lambda p, q: p + q, values)


def dot(lhs, rhs):
    return jnp.dot(lhs, rhs, preferred_element_type=F32)


def each(count, limit, step):
    if count <= limit:
        for number in range(count):
            step(number)
    else:
        lax.fori_loop(0, count, lambda number, carry: (step(number), carry)[1], 0)


def dot_across(lhs, rhs):
    return lax.dot_general(lhs, rhs, (((1,), (1,)), ((), ())), preferred_element_type=F32)


def pick(table, index):
    return jnp.take_along_axis(table, index, axis=1, mode="promise_in_bounds")


def fetch(pairs, sems):
    copies = [pltpu.make_async_copy(src, dst, sems.at[n]) for n, (src, dst) in enumerate(pairs)]
    for copy in copies:
        copy.start()
    return copies


def member(place, half):
    return (place + half - 1) % half


def order_of(spans, root, stride):
    return [(root + stride * n) % spans for n in range(spans)]


def halves(groups, order):
    half = groups // 2
    return [
        [span * groups + side * half + member(place, half) for span in order for place in range(half)]
        for side in range(2)
    ]


def coder(verts, block):
    shape = block * 6.0 * 0.3125 + 6.0
    limit = max(shape, verts * 0.5 * shape)
    unit = 2.0**-16
    rate = math.log1p(limit / unit) / 32766.0
    return unit, rate


def pack_kernel(groups, spans, coeffs_hbm, index_hbm, raw_hbm, out_ref, coeffs_s, index_s, raw_s, row_s, sems):
    copies = fetch([(coeffs_hbm, coeffs_s), (index_hbm, index_s), (raw_hbm, raw_s)], sems)
    own_chars, comps = coeffs_s.shape
    half = groups // 2
    block = comps // groups
    slots, verts = index_s.shape
    per_group = slots // half
    column = lax.rem(lax.axis_index("col"), half)
    side = lax.div(lax.axis_index("col"), half)
    row_s[...] = jnp.zeros_like(row_s)
    for copy in copies:
        copy.wait()
    wide = coeffs_s[...].astype(F32)
    index = index_s[...].astype(F32)
    raw = raw_s[...]
    for which in range(per_group):
        sel = lax.broadcasted_iota(jnp.int32, index.shape, 0) == column * per_group + which
        at = 2 * own_chars + 2 * which
        for more, value in enumerate((index, raw)):
            value = jnp.sum(jnp.where(sel, value, 0.0), axis=0, keepdims=True)
            for place in range(half):
                row_s[place, at + more : at + more + 1, 0:verts] = value
    for place in range(half):
        low = [(part * half + member(place, half)) * block for part in range(2)]
        low = [wide[:, at : at + block] for at in low]
        row_s[place, 0:own_chars, 0:block] = jnp.where(side == 0, low[0], low[1])
        row_s[place, own_chars : 2 * own_chars, 0:block] = jnp.where(side == 0, low[1], low[0])
    for place in range(half):
        value = row_s[place]
        for span in range(spans):
            out_ref[span * half + place] = value


def prep_kernel(
    half,
    basis_hbm,
    template_hbm,
    regressor_hbm,
    quat_hbm,
    move_hbm,
    parents_hbm,
    own_ref,
    temp_ref,
    reg_ref,
    table_ref,
    diff_ref,
    above_ref,
    shift_ref,
    basis_s,
    template_s,
    regressor_s,
    quat_raw,
    move_s,
    parents_s,
    reg_s,
    quat_s,
    parent_s,
    sems,
):
    copies = fetch(
        [
            (basis_hbm, basis_s),
            (template_hbm, template_s),
            (regressor_hbm, regressor_s),
            (quat_hbm, quat_raw),
            (move_hbm, move_s),
            (parents_hbm, parents_s),
        ],
        sems,
    )
    _, verts, block = basis_s.shape
    own_chars, _, joints = quat_raw.shape
    start, first, rest, step = layout(verts, joints)
    lane = lax.broadcasted_iota(jnp.int32, (SUBS, LANES), 1)
    sub = lax.broadcasted_iota(jnp.int32, (SUBS, LANES), 0)
    row = sub // own_chars
    char_of = sub % own_chars

    def by_char(rows):
        value = jnp.broadcast_to(rows[0], (SUBS, LANES))
        for char in range(1, own_chars):
            value = jnp.where(char_of == char, rows[char], value)
        return value

    def by_row(values):
        value = values[-1]
        for n in range(len(values) - 2, -1, -1):
            value = jnp.where(row == n, values[n], value)
        return value

    own_ref[...] = jnp.zeros_like(own_ref)
    temp_ref[...] = jnp.zeros_like(temp_ref)
    reg_s[...] = jnp.zeros_like(reg_s)
    quat_s[...] = jnp.zeros_like(quat_s)
    quat_s[:, 0:1, :] = jnp.ones_like(quat_s[:, 0:1, :])
    parent_s[...] = jnp.zeros_like(parent_s)
    for copy in copies:
        copy.wait()
    for coord in range(3):
        own_ref[coord, 0:verts, 0:block] = basis_s[coord]
    temp_ref[0:3, 0:verts] = template_s[...] * (1.0 / half)
    reg_s[start:LANES, 0:verts] = regressor_s[0:first, :]
    reg_s[LANES : LANES + rest, 0:verts] = regressor_s[first:joints, :]
    high, low = split_two(reg_s[...])
    for n, value in enumerate((high, low, high)):
        reg_ref[:, n * LANES : (n + 1) * LANES] = value

    quat_s[:, :, 0:joints] = quat_raw[...]
    w, x, y, z = [
        by_char([quat_s[char, comp : comp + 1, :] for char in range(own_chars)]) for comp in range(4)
    ]
    two = 2.0 / (w * w + x * x + y * y + z * z)
    rot = [
        by_row([1.0 - two * (y * y + z * z), two * (x * y + w * z), two * (x * z - w * y)]),
        by_row([two * (x * y - w * z), 1.0 - two * (x * x + z * z), two * (y * z + w * x)]),
        by_row([two * (x * z + w * y), two * (y * z - w * x), 1.0 - two * (x * x + y * y)]),
    ]
    parent_s[0:1, 0:joints] = parents_s[...]
    parent = jnp.broadcast_to(parent_s[0:1, :], (SUBS, LANES))
    parent = jnp.where((lane >= joints) | (lane == 0), joints, parent)

    wide = round_up(joints, SUBS)
    spot = lax.broadcasted_iota(jnp.int32, (wide, LANES), 0)
    target = lax.broadcasted_iota(jnp.int32, (wide, LANES), 1)
    chain = jnp.where((spot == target) & (target < joints), 1.0, 0.0)
    chain = [chain[n : n + SUBS] for n in range(0, wide, SUBS)]
    above = parent
    levels = max(1, (joints - 1).bit_length())
    for level in range(levels):
        spread = []
        for b in range(3):
            turned = [rot[b]] + [pltpu.roll(rot[b], n * own_chars, 0) for n in range(1, 4)]
            spread.append([by_row([turned[(r - m) % 4] for r in range(3)]) for m in range(3)])
        up = [pick(rot[b], above) for b in range(3)]
        rot = [sum_of([up[m] * spread[b][m] for m in range(3)]) for b in range(3)]
        chain = [value + pick(value, above) for value in chain]
        if level + 1 < levels:
            above = pick(above, above)

    for turn in range(3):
        table_ref[turn] = by_row([rot[(a + turn) % 3] for a in range(3)])
    far = jnp.zeros((SUBS, LANES), F32)
    for coord in range(3):
        diff = pick(rot[coord], parent) - rot[coord]
        diff_ref[coord] = jnp.where(lane >= start, pltpu.roll(diff, start, 1), 0.0)
        turned = pltpu.roll(diff, (coord * step - first) % LANES, 1)
        far = jnp.where((lane >= coord * step) & (lane < coord * step + rest), turned, far)
    diff_ref[3] = far
    none = jnp.zeros((SUBS, LANES), F32)
    tail = chain[first // SUBS :]
    tail = tail + [none] * (step // SUBS - len(tail))
    body = chain[: first // SUBS]
    middle = [none] * ((start - 3 * step) // SUBS)
    above_ref[...] = jnp.concatenate(tail * 3 + middle + body, axis=0).astype(BF16)
    moved = none
    for char in range(own_chars):
        for a in range(3):
            moved = jnp.where(sub == a * own_chars + char, move_s[char : char + 1, a : a + 1], moved)
    shift_ref[...] = moved


def shape_kernel(
    half,
    own_chars,
    verts,
    slots,
    joints,
    order,
    next_order,
    flat_ref,
    other_ref,
    own_ref,
    temp_ref,
    reg_ref,
    table_ref,
    out_ref,
    index_ref,
    share_ref,
    coef_ref,
    pad_s,
    skin_s,
    sum_s,
):
    block = other_ref.shape[2]
    height = 2 * own_chars + 2 * slots // half
    count = flat_ref.shape[0] // height
    spans = count // half
    step = layout(verts, joints)[3]

    pad_s[...] = jnp.zeros_like(pad_s)
    for coord in range(3):
        pad_s[coord, 0:verts, 0:block] = other_ref[coord]
    chunk = min(16, count)
    total = own_chars * chunk
    unit, rate = coder(verts, 2 * block)

    def do_chunk(number):
        at = number * chunk * height
        coeffs = jnp.concatenate(
            [
                jnp.concatenate(
                    [
                        flat_ref[pl.ds(at + part * own_chars + char, chunk, stride=height), :]
                        for char in range(own_chars)
                    ],
                    axis=0,
                )
                for part in range(2)
            ],
            axis=1,
        ).astype(BF16)
        shapes = [
            dot_across(coeffs, jnp.concatenate([own_ref[coord], pad_s[coord]], axis=1))
            + temp_ref[coord : coord + 1, :]
            for coord in range(3)
        ]
        high, low = split_two(jnp.concatenate(shapes, axis=0))
        sums = dot_across(jnp.concatenate([high, high, low], axis=1), reg_ref[...])
        last = sums[0:total, LANES:]
        for coord in range(1, 3):
            last = last + pltpu.roll(sums[coord * total : (coord + 1) * total, LANES:], coord * step, 1)
        rows = [shapes[coord] + sums[coord * total : (coord + 1) * total, :LANES] for coord in range(3)]
        for place, value in enumerate(rows + [last]):
            code = jnp.log(1.0 + jnp.abs(value) * (1.0 / unit)) * (1.0 / rate)
            code = jnp.where(value < 0.0, -code, code)
            for char in range(own_chars):
                sum_s[pl.ds(number * chunk, chunk), place * own_chars + char, :] = code[
                    char * chunk : (char + 1) * chunk
                ]

    each(count // chunk, 1, do_chunk)
    for n, span in enumerate(next_order):
        at = order.index(span) * half
        out_ref[n * half : (n + 1) * half] = (
            jnp.round(sum_s[at : at + half]).astype(jnp.int32).astype(jnp.int16)
        )

    per_group = slots // half
    for base in range(0, spans, SUBS):
        many = min(SUBS, spans - base)
        rows = [None] * (2 * slots)
        for place in range(half):
            for more in range(2 * per_group):
                at = (base * half + place) * height + 2 * own_chars + more
                rows[2 * per_group * member(place, half) + more] = flat_ref[
                    pl.ds(at, many, stride=half * height), :
                ]
        scale = 1.0 / sum_of(rows[1::2])
        rows[1::2] = [value * scale for value in rows[1::2]]
        for n, value in enumerate(rows):
            skin_s[pl.ds(base * 2 * slots + n, many, stride=2 * slots), :] = value
    tiles = index_ref.shape[1] // LANES
    values = [None] * tiles
    wide_lane = lax.broadcasted_iota(jnp.int32, (2 * slots, LANES), 1)
    for span in range(spans):
        at = order.index(span) * 2 * slots
        value = skin_s[at : at + 2 * slots, :]
        low = span * verts
        value = pltpu.roll(value, low % LANES, 1) if low % LANES else value
        for tile in range(low // LANES, (low + verts - 1) // LANES + 1):
            begin = low - tile * LANES
            values[tile] = value if begin <= 0 else jnp.where(wide_lane >= begin, value, values[tile])
    for tile in range(tiles):
        at = slice(tile * LANES, (tile + 1) * LANES)
        index_ref[:, at] = values[tile].astype(jnp.int32)
        share_ref[:, at] = values[tile]
        coef = [None] * 3
        for n in range(slots):
            wide = jnp.broadcast_to(values[tile][2 * n : 2 * n + 1, :], (SUBS, LANES)).astype(jnp.int32)
            share = values[tile][2 * n + 1 : 2 * n + 2, :]
            terms = [share * pick(table_ref[part], wide) for part in range(3)]
            coef = terms if n == 0 else [coef[part] + terms[part] for part in range(3)]
        for part in range(3):
            coef_ref[part, :, at] = coef[part]


def pose_kernel(
    half,
    order,
    own_chars,
    verts,
    block,
    recv_ref,
    diff_ref,
    above_ref,
    shift_ref,
    index_ref,
    share_ref,
    coef_ref,
    out_ref,
    total_s,
):
    spans = recv_ref.shape[0] // half
    slots = index_ref.shape[0] // 2
    width = out_ref.shape[2]
    tiles = -(-width // LANES)
    lane = lax.broadcasted_iota(jnp.int32, (SUBS, LANES), 1)
    sub = lax.broadcasted_iota(jnp.int32, (SUBS, LANES), 0)
    row = sub // own_chars
    char_of = sub % own_chars
    unit, rate = coder(verts, 2 * block)

    def decode(number):
        code = recv_ref[number].astype(jnp.int32).astype(F32)
        value = jnp.exp(jnp.abs(code) * rate) * unit - unit
        return jnp.where(code < 0.0, -value, value)

    total = None
    shapes = [None] * tiles
    for span in range(spans):
        at = order.index(span) * half
        value = sum_of([decode(at + place) for place in range(half)])
        total = value if total is None else total + value
        low = span * verts
        turned = pltpu.roll(value, low % LANES, 1) if low % LANES else value
        for tile in range(low // LANES, (low + verts - 1) // LANES + 1):
            begin = low - tile * LANES
            shapes[tile] = turned if begin <= 0 else jnp.where(lane >= begin, turned, shapes[tile])

    total_s[...] = total
    terms = []
    for coord in range(4):
        pair = jnp.broadcast_to(total_s[coord * own_chars : coord * own_chars + 1, :], (SUBS, LANES))
        for char in range(1, own_chars):
            at = coord * own_chars + char
            pair = jnp.where(char_of == char, total_s[at : at + 1, :], pair)
        terms.append(diff_ref[coord] * pair)
    lhs = (terms[0] + terms[1]) + (terms[2] + terms[3])
    high = lhs.astype(BF16).astype(F32)
    moved = dot(jnp.concatenate([high, lhs - high], axis=0).astype(BF16), above_ref[...])
    moved = (moved[:SUBS] + moved[SUBS:]) + shift_ref[...]
    for tile in range(tiles):
        end = min(width, (tile + 1) * LANES)
        at = slice(tile * LANES, (tile + 1) * LANES)
        index = [jnp.broadcast_to(index_ref[2 * n : 2 * n + 1, at], (SUBS, LANES)) for n in range(slots)]
        share = [share_ref[2 * n + 1 : 2 * n + 2, at] for n in range(slots)]
        shape = shapes[tile].astype(BF16).astype(F32)
        by_one = pltpu.roll(shape, own_chars, 0)
        by_two = pltpu.roll(shape, 2 * own_chars, 0)
        by_three = pltpu.roll(shape, 3 * own_chars, 0)
        turned = (
            coef_ref[0, :, at] * shape
            + coef_ref[1, :, at] * jnp.where(row < 2, by_three, by_two)
            + coef_ref[2, :, at] * jnp.where(row < 1, by_two, by_one)
        )
        posed = turned + sum_of([share[n] * pick(moved, index[n]) for n in range(slots)])
        for a in range(3):
            out_ref[a, :, tile * LANES : end] = posed[
                a * own_chars : (a + 1) * own_chars, : end - tile * LANES
            ].astype(BF16)


def body(spans, groups, coeffs, shape_basis, template, regressor, quaternions, translation, parents, skin_index, skin_raw):
    own_chars, comps = coeffs.shape
    verts, slots = skin_index.shape
    joints = regressor.shape[0]
    half = groups // 2
    members = spans * half
    block = comps // groups
    rows = 2 * own_chars + 2 * slots // half
    orders = (order_of(spans, spans // 2 - 1, 5), order_of(spans, spans // 2 + 1, 5))
    padded = round_up(spans * verts, LANES)
    whole = jax.ShapeDtypeStruct
    room = pltpu.CompilerParams(vmem_limit_bytes=16 * 2**20)
    basis = shape_basis.transpose(1, 2, 0)
    other = lax.ppermute(basis, "col", [(n, (n + half) % groups) for n in range(groups)])

    def exchange(value, order):
        return lax.all_to_all(
            value, ("vert", "col"), 0, 0, tiled=True, axis_index_groups=halves(groups, order)
        )

    message = pl.pallas_call(
        functools.partial(pack_kernel, groups, spans),
        out_shape=whole((members, rows, LANES), F32),
        in_specs=[HBM] * 3,
        out_specs=VMEM,
        scratch_shapes=[
            pltpu.VMEM((own_chars, comps), BF16),
            pltpu.VMEM((slots, verts), jnp.int32),
            pltpu.VMEM((slots, verts), F32),
            pltpu.VMEM((half, rows, LANES), F32),
            pltpu.SemaphoreType.DMA((3,)),
        ],
        compiler_params=room,
        name="pack",
    )(*in_hbm(coeffs, skin_index.T, skin_raw.T))
    received = exchange(message, orders[0])
    own, temp, reg, table, *local = pl.pallas_call(
        functools.partial(prep_kernel, half),
        out_shape=[
            whole((3, LANES, LANES), BF16),
            whole((SUBS, LANES), F32),
            whole((2 * LANES, 3 * LANES), BF16),
            whole((3, SUBS, LANES), F32),
            whole((4, SUBS, LANES), F32),
            whole((LANES, LANES), BF16),
            whole((SUBS, LANES), F32),
        ],
        in_specs=[HBM] * 6,
        out_specs=[VMEM] * 7,
        scratch_shapes=[
            pltpu.VMEM((3, verts, block), BF16),
            pltpu.VMEM((3, verts), F32),
            pltpu.VMEM((joints, verts), F32),
            pltpu.VMEM((own_chars, 4, joints), F32),
            pltpu.VMEM((own_chars, 3), F32),
            pltpu.VMEM((1, joints), jnp.int32),
            pltpu.VMEM((2 * LANES, LANES), F32),
            pltpu.VMEM((own_chars, 4, LANES), F32),
            pltpu.VMEM((SUBS, LANES), jnp.int32),
            pltpu.SemaphoreType.DMA((6,)),
        ],
        compiler_params=room,
        cost_estimate=pl.CostEstimate(flops=10**7, bytes_accessed=10**6, transcendentals=0),
        name="prep",
    )(*in_hbm(basis, template, regressor, quaternions, translation, parents.reshape(1, joints)))
    partials, *skin = pl.pallas_call(
        functools.partial(shape_kernel, half, own_chars, verts, slots, joints, *orders),
        out_shape=[
            whole((members, 4 * own_chars, LANES), jnp.int16),
            whole((2 * slots, padded), jnp.int32),
            whole((2 * slots, padded), F32),
            whole((3, SUBS, padded), F32),
        ],
        in_specs=[VMEM] * 6,
        out_specs=[VMEM] * 4,
        scratch_shapes=[
            pltpu.VMEM((3, LANES, LANES), BF16),
            pltpu.VMEM((spans * 2 * slots, LANES), F32),
            pltpu.VMEM((members, 4 * own_chars, LANES), F32),
        ],
        compiler_params=room,
        name="shape",
    )(received.reshape(members * rows, LANES), other, own, temp, reg, table)
    received = exchange(partials, orders[1])
    posed = pl.pallas_call(
        functools.partial(pose_kernel, half, orders[1], own_chars, verts, block),
        out_shape=whole((3, own_chars, spans * verts), BF16),
        in_specs=[VMEM] * 7,
        out_specs=VMEM,
        scratch_shapes=[pltpu.VMEM((SUBS, LANES), F32)],
        compiler_params=room,
        name="pose",
    )(received, *local, *skin)
    return posed.transpose(1, 0, 2)


def solution(mesh):
    in_specs = (
        P(("vert", "col"), None),
        P("col", None, "vert"),
        P(None, "vert"),
        P(None, "vert"),
        P(("vert", "col"), None, None),
        P(("vert", "col"), None),
        P(),
        P("vert", None),
        P("vert", None),
    )
    out_specs = P(("vert", "col"), None, None)
    return jax.shard_map(
        functools.partial(body, mesh.shape["vert"], mesh.shape["col"]),
        mesh=mesh,
        in_specs=in_specs,
        out_specs=out_specs,
        check_vma=False,
    )
```

```python
import functools
import math

import jax
import jax.numpy as jnp
from jax import lax
from jax.experimental import pallas as pl
from jax.experimental.pallas import tpu as pltpu
from jax.sharding import PartitionSpec as P

LANES = 128
SUBS = 8
VMEM = pl.BlockSpec(memory_space=pltpu.VMEM)
HBM = pl.BlockSpec(memory_space=pltpu.HBM)
F32 = jnp.float32
BF16 = jnp.bfloat16


def round_up(value, step):
    return -(-value // step) * step


def layout(verts, joints):
    start = round_up(verts, SUBS)
    first = LANES - start
    rest = joints - first
    step = round_up(rest, SUBS)
    return start, first, rest, step


def in_hbm(*values):
    return [pltpu.with_memory_space_constraint(value, pltpu.HBM) for value in values]


def split_two(value):
    high = value.astype(BF16)
    return high, (value - high.astype(F32)).astype(BF16)


def sum_of(values):
    values = list(values)
    while len(values) > 1:
        values = [sum(values[n + 1 : n + 2], values[n]) for n in range(0, len(values), 2)]
    return values[0]


def dot(lhs, rhs):
    return jnp.dot(lhs, rhs, preferred_element_type=F32)


def each(count, limit, step):
    if count <= limit:
        for number in range(count):
            step(number)
    else:
        lax.fori_loop(0, count, lambda number, carry: (step(number), carry)[1], 0)


def dot_across(lhs, rhs):
    return lax.dot_general(lhs, rhs, (((1,), (1,)), ((), ())), preferred_element_type=F32)


def pick(table, index):
    return jnp.take_along_axis(table, index, axis=1, mode="promise_in_bounds")


def fetch(pairs, sems):
    copies = [pltpu.make_async_copy(src, dst, sems.at[n]) for n, (src, dst) in enumerate(pairs)]
    for copy in copies:
        copy.start()
    return copies


def member(place, half):
    return (place + half - 1) % half


def order_of(spans, root, stride):
    return [(root + stride * n) % spans for n in range(spans)]


def halves(groups, order):
    half = groups // 2
    return [
        [span * groups + side * half + member(place, half) for span in order for place in range(half)]
        for side in range(2)
    ]


def coder(verts, block):
    shape = block * 6.0 * 0.3125 + 6.0
    limit = max(shape, verts * 0.5 * shape)
    unit = 2.0**-16
    rate = math.log1p(limit / unit) / 32766.0
    return unit, rate


def pack_kernel(groups, spans, coeffs_hbm, index_hbm, raw_hbm, out_ref, coeffs_s, index_s, raw_s, row_s, sems):
    copies = fetch([(coeffs_hbm, coeffs_s), (index_hbm, index_s), (raw_hbm, raw_s)], sems)
    own_chars, comps = coeffs_s.shape
    half = groups // 2
    block = comps // groups
    slots, verts = index_s.shape
    per_group = slots // half
    column = lax.rem(lax.axis_index("col"), half)
    side = lax.div(lax.axis_index("col"), half)
    row_s[...] = jnp.zeros_like(row_s)
    for copy in copies:
        copy.wait()
    wide = coeffs_s[...].astype(F32)
    index = index_s[...].astype(F32)
    raw = raw_s[...]
    for which in range(per_group):
        sel = lax.broadcasted_iota(jnp.int32, index.shape, 0) == column * per_group + which
        at = 2 * own_chars + 2 * which
        for more, value in enumerate((index, raw)):
            value = jnp.sum(jnp.where(sel, value, 0.0), axis=0, keepdims=True)
            for place in range(half):
                row_s[place, at + more : at + more + 1, 0:verts] = value
    for place in range(half):
        low = [(part * half + member(place, half)) * block for part in range(2)]
        low = [wide[:, at : at + block] for at in low]
        row_s[place, 0:own_chars, 0:block] = jnp.where(side == 0, low[0], low[1])
        row_s[place, own_chars : 2 * own_chars, 0:block] = jnp.where(side == 0, low[1], low[0])
    for place in range(half):
        value = row_s[place]
        for span in range(spans):
            out_ref[span * half + place] = value


def prep_kernel(
    half,
    basis_hbm,
    template_hbm,
    regressor_hbm,
    quat_hbm,
    move_hbm,
    parents_hbm,
    own_ref,
    temp_ref,
    reg_ref,
    table_ref,
    diff_ref,
    above_ref,
    shift_ref,
    basis_s,
    template_s,
    regressor_s,
    quat_raw,
    move_s,
    parents_s,
    reg_s,
    quat_s,
    parent_s,
    sems,
):
    copies = fetch(
        [
            (basis_hbm, basis_s),
            (template_hbm, template_s),
            (regressor_hbm, regressor_s),
            (quat_hbm, quat_raw),
            (move_hbm, move_s),
            (parents_hbm, parents_s),
        ],
        sems,
    )
    _, verts, block = basis_s.shape
    own_chars, _, joints = quat_raw.shape
    start, first, rest, step = layout(verts, joints)
    lane = lax.broadcasted_iota(jnp.int32, (SUBS, LANES), 1)
    sub = lax.broadcasted_iota(jnp.int32, (SUBS, LANES), 0)
    row = sub // own_chars
    char_of = sub % own_chars

    def by_char(rows):
        value = jnp.broadcast_to(rows[0], (SUBS, LANES))
        for char in range(1, own_chars):
            value = jnp.where(char_of == char, rows[char], value)
        return value

    def by_row(values):
        value = values[-1]
        for n in range(len(values) - 2, -1, -1):
            value = jnp.where(row == n, values[n], value)
        return value

    own_ref[...] = jnp.zeros_like(own_ref)
    temp_ref[...] = jnp.zeros_like(temp_ref)
    reg_s[...] = jnp.zeros_like(reg_s)
    quat_s[...] = jnp.zeros_like(quat_s)
    quat_s[:, 0:1, :] = jnp.ones_like(quat_s[:, 0:1, :])
    parent_s[...] = jnp.zeros_like(parent_s)
    for copy in copies:
        copy.wait()
    for coord in range(3):
        own_ref[coord, 0:verts, 0:block] = basis_s[coord]
    temp_ref[0:3, 0:verts] = template_s[...] * (1.0 / half)
    reg_s[start:LANES, 0:verts] = regressor_s[0:first, :]
    for coord in range(3):
        at = LANES + coord * step
        reg_s[at : at + rest, 0:verts] = regressor_s[first:joints, :]
    high, low = split_two(reg_s[...])
    for n, value in enumerate((high, low, high)):
        reg_ref[:, n * LANES : (n + 1) * LANES] = value

    quat_s[:, :, 0:joints] = quat_raw[...]
    w, x, y, z = [
        by_char([quat_s[char, comp : comp + 1, :] for char in range(own_chars)]) for comp in range(4)
    ]
    two = 2.0 / (w * w + x * x + y * y + z * z)
    rot = [
        by_row([1.0 - two * (y * y + z * z), two * (x * y + w * z), two * (x * z - w * y)]),
        by_row([two * (x * y - w * z), 1.0 - two * (x * x + z * z), two * (y * z + w * x)]),
        by_row([two * (x * z + w * y), two * (y * z - w * x), 1.0 - two * (x * x + y * y)]),
    ]
    parent_s[0:1, 0:joints] = parents_s[...]
    parent = jnp.broadcast_to(parent_s[0:1, :], (SUBS, LANES))
    parent = jnp.where((lane >= joints) | (lane == 0), joints, parent)

    wide = round_up(joints, SUBS)
    spot = lax.broadcasted_iota(jnp.int32, (wide, LANES), 0)
    target = lax.broadcasted_iota(jnp.int32, (wide, LANES), 1)
    chain = jnp.where((spot == target) & (target < joints), 1.0, 0.0)
    chain = [chain[n : n + SUBS] for n in range(0, wide, SUBS)]
    above = parent
    levels = max(1, (joints - 1).bit_length())
    for level in range(levels):
        spread = []
        for b in range(3):
            turned = [rot[b]] + [pltpu.roll(rot[b], n * own_chars, 0) for n in range(1, 4)]
            spread.append([by_row([turned[(r - m) % 4] for r in range(3)]) for m in range(3)])
        up = [pick(rot[b], above) for b in range(3)]
        rot = [sum_of([up[m] * spread[b][m] for m in range(3)]) for b in range(3)]
        chain = [value + pick(value, above) for value in chain]
        if level + 1 < levels:
            above = pick(above, above)

    for turn in range(3):
        table_ref[turn] = by_row([rot[(a + turn) % 3] for a in range(3)])
    far = jnp.zeros((SUBS, LANES), F32)
    for coord in range(3):
        diff = pick(rot[coord], parent) - rot[coord]
        diff_ref[coord] = jnp.where(lane >= start, pltpu.roll(diff, start, 1), 0.0)
        turned = pltpu.roll(diff, (coord * step - first) % LANES, 1)
        far = jnp.where((lane >= coord * step) & (lane < coord * step + rest), turned, far)
    diff_ref[3] = far
    none = jnp.zeros((SUBS, LANES), F32)
    tail = chain[first // SUBS :]
    tail = tail + [none] * (step // SUBS - len(tail))
    body = chain[: first // SUBS]
    middle = [none] * ((start - 3 * step) // SUBS)
    above_ref[...] = jnp.concatenate(tail * 3 + middle + body, axis=0).astype(BF16)
    moved = none
    for char in range(own_chars):
        for a in range(3):
            moved = jnp.where(sub == a * own_chars + char, move_s[char : char + 1, a : a + 1], moved)
    shift_ref[...] = moved


def shape_kernel(
    half,
    own_chars,
    verts,
    slots,
    joints,
    order,
    next_order,
    flat_ref,
    other_ref,
    own_ref,
    temp_ref,
    reg_ref,
    table_ref,
    out_ref,
    index_ref,
    share_ref,
    coef_ref,
    pad_s,
    skin_s,
    sum_s,
):
    block = other_ref.shape[2]
    height = 2 * own_chars + 2 * slots // half
    count = flat_ref.shape[0] // height
    spans = count // half
    step = layout(verts, joints)[3]

    pad_s[...] = jnp.zeros_like(pad_s)
    for coord in range(3):
        pad_s[coord, 0:verts, 0:block] = other_ref[coord]
    chunk = min(16, count)
    total = own_chars * chunk
    rows_lane = lax.broadcasted_iota(jnp.int32, (total, LANES), 1)
    unit, rate = coder(verts, 2 * block)

    def do_chunk(number):
        at = number * chunk * height
        coeffs = jnp.concatenate(
            [
                jnp.concatenate(
                    [
                        flat_ref[pl.ds(at + part * own_chars + char, chunk, stride=height), :]
                        for char in range(own_chars)
                    ],
                    axis=0,
                )
                for part in range(2)
            ],
            axis=1,
        ).astype(BF16)
        shapes = [
            dot_across(coeffs, jnp.concatenate([own_ref[coord], pad_s[coord]], axis=1))
            + temp_ref[coord : coord + 1, :]
            for coord in range(3)
        ]
        high, low = split_two(jnp.concatenate(shapes, axis=0))
        sums = dot_across(jnp.concatenate([high, high, low], axis=1), reg_ref[...])
        last = sums[2 * total : 3 * total, LANES:]
        for coord in (1, 0):
            last = jnp.where(
                rows_lane < (coord + 1) * step, sums[coord * total : (coord + 1) * total, LANES:], last
            )
        rows = [shapes[coord] + sums[coord * total : (coord + 1) * total, :LANES] for coord in range(3)]
        for place, value in enumerate(rows + [last]):
            code = jnp.log(1.0 + jnp.abs(value) * (1.0 / unit)) * (1.0 / rate)
            code = jnp.where(value < 0.0, -code, code)
            for char in range(own_chars):
                sum_s[pl.ds(number * chunk, chunk), place * own_chars + char, :] = code[
                    char * chunk : (char + 1) * chunk
                ]

    each(count // chunk, 1, do_chunk)
    for n, span in enumerate(next_order):
        at = order.index(span) * half
        out_ref[n * half : (n + 1) * half] = (
            jnp.round(sum_s[at : at + half]).astype(jnp.int32).astype(jnp.int16)
        )

    per_group = slots // half
    for base in range(0, spans, SUBS):
        many = min(SUBS, spans - base)
        rows = [None] * (2 * slots)
        for place in range(half):
            for more in range(2 * per_group):
                at = (base * half + place) * height + 2 * own_chars + more
                rows[2 * per_group * member(place, half) + more] = flat_ref[
                    pl.ds(at, many, stride=half * height), :
                ]
        scale = 1.0 / sum_of(rows[1::2])
        rows[1::2] = [value * scale for value in rows[1::2]]
        for n, value in enumerate(rows):
            skin_s[pl.ds(base * 2 * slots + n, many, stride=2 * slots), :] = value
    tiles = index_ref.shape[1] // LANES
    values = [None] * tiles
    wide_lane = lax.broadcasted_iota(jnp.int32, (2 * slots, LANES), 1)
    for span in range(spans):
        at = order.index(span) * 2 * slots
        value = skin_s[at : at + 2 * slots, :]
        low = span * verts
        value = pltpu.roll(value, low % LANES, 1) if low % LANES else value
        for tile in range(low // LANES, (low + verts - 1) // LANES + 1):
            begin = low - tile * LANES
            values[tile] = value if begin <= 0 else jnp.where(wide_lane >= begin, value, values[tile])
    for tile in range(tiles):
        at = slice(tile * LANES, (tile + 1) * LANES)
        index_ref[:, at] = values[tile].astype(jnp.int32)
        share_ref[:, at] = values[tile]
        coef = [None] * 3
        for n in range(slots):
            wide = jnp.broadcast_to(values[tile][2 * n : 2 * n + 1, :], (SUBS, LANES)).astype(jnp.int32)
            share = values[tile][2 * n + 1 : 2 * n + 2, :]
            terms = [share * pick(table_ref[part], wide) for part in range(3)]
            coef = terms if n == 0 else [coef[part] + terms[part] for part in range(3)]
        for part in range(3):
            coef_ref[part, :, at] = coef[part]


def pose_kernel(
    half,
    order,
    own_chars,
    verts,
    block,
    recv_ref,
    diff_ref,
    above_ref,
    shift_ref,
    index_ref,
    share_ref,
    coef_ref,
    out_ref,
    total_s,
):
    spans = recv_ref.shape[0] // half
    slots = index_ref.shape[0] // 2
    width = out_ref.shape[2]
    tiles = -(-width // LANES)
    lane = lax.broadcasted_iota(jnp.int32, (SUBS, LANES), 1)
    sub = lax.broadcasted_iota(jnp.int32, (SUBS, LANES), 0)
    row = sub // own_chars
    char_of = sub % own_chars
    unit, rate = coder(verts, 2 * block)

    def decode(number):
        code = recv_ref[number].astype(jnp.int32).astype(F32)
        value = jnp.exp(jnp.abs(code) * rate) * unit - unit
        return jnp.where(code < 0.0, -value, value)

    parts = []
    shapes = [None] * tiles
    for span in range(spans):
        at = order.index(span) * half
        value = sum_of([decode(at + place) for place in range(half)])
        parts.append(value)
        low = span * verts
        turned = pltpu.roll(value, low % LANES, 1) if low % LANES else value
        for tile in range(low // LANES, (low + verts - 1) // LANES + 1):
            begin = low - tile * LANES
            shapes[tile] = turned if begin <= 0 else jnp.where(lane >= begin, turned, shapes[tile])

    total_s[...] = sum_of(parts)
    terms = []
    for coord in range(4):
        pair = jnp.broadcast_to(total_s[coord * own_chars : coord * own_chars + 1, :], (SUBS, LANES))
        for char in range(1, own_chars):
            at = coord * own_chars + char
            pair = jnp.where(char_of == char, total_s[at : at + 1, :], pair)
        terms.append(diff_ref[coord] * pair)
    lhs = (terms[0] + terms[1]) + (terms[2] + terms[3])
    high = lhs.astype(BF16).astype(F32)
    moved = dot(jnp.concatenate([high, lhs - high], axis=0).astype(BF16), above_ref[...])
    moved = (moved[:SUBS] + moved[SUBS:]) + shift_ref[...]
    for tile in range(tiles):
        end = min(width, (tile + 1) * LANES)
        at = slice(tile * LANES, (tile + 1) * LANES)
        index = [jnp.broadcast_to(index_ref[2 * n : 2 * n + 1, at], (SUBS, LANES)) for n in range(slots)]
        share = [share_ref[2 * n + 1 : 2 * n + 2, at] for n in range(slots)]
        shape = shapes[tile].astype(BF16).astype(F32)
        by_one = pltpu.roll(shape, own_chars, 0)
        by_two = pltpu.roll(shape, 2 * own_chars, 0)
        by_three = pltpu.roll(shape, 3 * own_chars, 0)
        turned = (
            coef_ref[0, :, at] * shape
            + coef_ref[1, :, at] * jnp.where(row < 2, by_three, by_two)
            + coef_ref[2, :, at] * jnp.where(row < 1, by_two, by_one)
        )
        posed = turned + sum_of([share[n] * pick(moved, index[n]) for n in range(slots)])
        for a in range(3):
            out_ref[a, :, tile * LANES : end] = posed[
                a * own_chars : (a + 1) * own_chars, : end - tile * LANES
            ].astype(BF16)


def body(spans, groups, coeffs, shape_basis, template, regressor, quaternions, translation, parents, skin_index, skin_raw):
    own_chars, comps = coeffs.shape
    verts, slots = skin_index.shape
    joints = regressor.shape[0]
    half = groups // 2
    members = spans * half
    block = comps // groups
    rows = 2 * own_chars + 2 * slots // half
    orders = (order_of(spans, spans // 2 - 1, 5), order_of(spans, spans // 2 + 1, 5))
    padded = round_up(spans * verts, LANES)
    whole = jax.ShapeDtypeStruct
    room = pltpu.CompilerParams(vmem_limit_bytes=16 * 2**20)
    basis = shape_basis.transpose(1, 2, 0)
    other = lax.ppermute(basis, "col", [(n, (n + half) % groups) for n in range(groups)])

    def exchange(value, order):
        return lax.all_to_all(
            value, ("vert", "col"), 0, 0, tiled=True, axis_index_groups=halves(groups, order)
        )

    message = pl.pallas_call(
        functools.partial(pack_kernel, groups, spans),
        out_shape=whole((members, rows, LANES), F32),
        in_specs=[HBM] * 3,
        out_specs=VMEM,
        scratch_shapes=[
            pltpu.VMEM((own_chars, comps), BF16),
            pltpu.VMEM((slots, verts), jnp.int32),
            pltpu.VMEM((slots, verts), F32),
            pltpu.VMEM((half, rows, LANES), F32),
            pltpu.SemaphoreType.DMA((3,)),
        ],
        compiler_params=room,
        name="pack",
    )(*in_hbm(coeffs, skin_index.T, skin_raw.T))
    received = exchange(message, orders[0])
    own, temp, reg, table, *local = pl.pallas_call(
        functools.partial(prep_kernel, half),
        out_shape=[
            whole((3, LANES, LANES), BF16),
            whole((SUBS, LANES), F32),
            whole((2 * LANES, 3 * LANES), BF16),
            whole((3, SUBS, LANES), F32),
            whole((4, SUBS, LANES), F32),
            whole((LANES, LANES), BF16),
            whole((SUBS, LANES), F32),
        ],
        in_specs=[HBM] * 6,
        out_specs=[VMEM] * 7,
        scratch_shapes=[
            pltpu.VMEM((3, verts, block), BF16),
            pltpu.VMEM((3, verts), F32),
            pltpu.VMEM((joints, verts), F32),
            pltpu.VMEM((own_chars, 4, joints), F32),
            pltpu.VMEM((own_chars, 3), F32),
            pltpu.VMEM((1, joints), jnp.int32),
            pltpu.VMEM((2 * LANES, LANES), F32),
            pltpu.VMEM((own_chars, 4, LANES), F32),
            pltpu.VMEM((SUBS, LANES), jnp.int32),
            pltpu.SemaphoreType.DMA((6,)),
        ],
        compiler_params=room,
        cost_estimate=pl.CostEstimate(flops=10**7, bytes_accessed=10**6, transcendentals=0),
        name="prep",
    )(*in_hbm(basis, template, regressor, quaternions, translation, parents.reshape(1, joints)))
    partials, *skin = pl.pallas_call(
        functools.partial(shape_kernel, half, own_chars, verts, slots, joints, *orders),
        out_shape=[
            whole((members, 4 * own_chars, LANES), jnp.int16),
            whole((2 * slots, padded), jnp.int32),
            whole((2 * slots, padded), F32),
            whole((3, SUBS, padded), F32),
        ],
        in_specs=[VMEM] * 6,
        out_specs=[VMEM] * 4,
        scratch_shapes=[
            pltpu.VMEM((3, LANES, LANES), BF16),
            pltpu.VMEM((spans * 2 * slots, LANES), F32),
            pltpu.VMEM((members, 4 * own_chars, LANES), F32),
        ],
        compiler_params=room,
        name="shape",
    )(received.reshape(members * rows, LANES), other, own, temp, reg, table)
    received = exchange(partials, orders[1])
    posed = pl.pallas_call(
        functools.partial(pose_kernel, half, orders[1], own_chars, verts, block),
        out_shape=whole((3, own_chars, spans * verts), BF16),
        in_specs=[VMEM] * 7,
        out_specs=VMEM,
        scratch_shapes=[pltpu.VMEM((SUBS, LANES), F32)],
        compiler_params=room,
        name="pose",
    )(received, *local, *skin)
    return posed.transpose(1, 0, 2)


def solution(mesh):
    in_specs = (
        P(("vert", "col"), None),
        P("col", None, "vert"),
        P(None, "vert"),
        P(None, "vert"),
        P(("vert", "col"), None, None),
        P(("vert", "col"), None),
        P(),
        P("vert", None),
        P("vert", None),
    )
    out_specs = P(("vert", "col"), None, None)
    return jax.shard_map(
        functools.partial(body, mesh.shape["vert"], mesh.shape["col"]),
        mesh=mesh,
        in_specs=in_specs,
        out_specs=out_specs,
        check_vma=False,
    )
```

```python
import functools
import math

import jax
import jax.numpy as jnp
from jax import lax
from jax.experimental import pallas as pl
from jax.experimental.pallas import tpu as pltpu
from jax.sharding import PartitionSpec as P

LANES = 128
SUBS = 8
VMEM = pl.BlockSpec(memory_space=pltpu.VMEM)
HBM = pl.BlockSpec(memory_space=pltpu.HBM)
F32 = jnp.float32
BF16 = jnp.bfloat16


def round_up(value, step):
    return -(-value // step) * step


def layout(verts, joints):
    start = round_up(verts, SUBS)
    first = LANES - start
    rest = joints - first
    step = round_up(rest, SUBS)
    return start, first, rest, step


def in_hbm(*values):
    return [pltpu.with_memory_space_constraint(value, pltpu.HBM) for value in values]


def split_two(value):
    high = value.astype(BF16)
    return high, (value - high.astype(F32)).astype(BF16)


def sum_of(values):
    values = list(values)
    while len(values) > 1:
        values = [sum(values[n + 1 : n + 2], values[n]) for n in range(0, len(values), 2)]
    return values[0]


def dot(lhs, rhs):
    return jnp.dot(lhs, rhs, preferred_element_type=F32)


def each(count, limit, step):
    if count <= limit:
        for number in range(count):
            step(number)
    else:
        lax.fori_loop(0, count, lambda number, carry: (step(number), carry)[1], 0)


def dot_across(lhs, rhs):
    return lax.dot_general(lhs, rhs, (((1,), (1,)), ((), ())), preferred_element_type=F32)


def pick(table, index):
    return jnp.take_along_axis(table, index, axis=1, mode="promise_in_bounds")


def fetch(pairs, sems):
    copies = [pltpu.make_async_copy(src, dst, sems.at[n]) for n, (src, dst) in enumerate(pairs)]
    for copy in copies:
        copy.start()
    return copies


def member(place, half):
    return (place + half - 1) % half


def order_of(spans, root, stride):
    return [(root + stride * n) % spans for n in range(spans)]


def halves(groups, order):
    half = groups // 2
    return [
        [span * groups + side * half + member(place, half) for span in order for place in range(half)]
        for side in range(2)
    ]


def coder(verts, block):
    shape = block * 6.0 * 0.3125 + 6.0
    limit = max(shape, verts * 0.5 * shape)
    unit = 2.0**-16
    rate = math.log2(1.0 + limit / unit) / 32766.0
    return unit, rate


def pack_kernel(groups, spans, coeffs_hbm, index_hbm, raw_hbm, out_ref, coeffs_s, index_s, raw_s, row_s, sems):
    copies = fetch([(coeffs_hbm, coeffs_s), (index_hbm, index_s), (raw_hbm, raw_s)], sems)
    own_chars, comps = coeffs_s.shape
    half = groups // 2
    block = comps // groups
    slots, verts = index_s.shape
    spare = LANES - verts
    per_group = slots // half
    column = lax.rem(lax.axis_index("col"), half)
    side = lax.div(lax.axis_index("col"), half)
    row_s[...] = jnp.zeros_like(row_s)
    for copy in copies:
        copy.wait()
    wide = coeffs_s[...].astype(F32)
    index = index_s[...].astype(F32)
    raw = raw_s[...]
    for which in range(per_group):
        sel = lax.broadcasted_iota(jnp.int32, index.shape, 0) == column * per_group + which
        value = [jnp.sum(jnp.where(sel, value, 0.0), axis=0, keepdims=True) for value in (index, raw)]
        high = value[1].astype(BF16).astype(F32)
        low = value[1] - high
        at = 2 * own_chars + 2 * which
        for place in range(half):
            row_s[place, at : at + 1, 0:verts] = value[0]
            row_s[place, at : at + 1, verts:LANES] = low[:, 0:spare]
            row_s[place, at + 1 : at + 2, 0:verts] = high
            row_s[place, at + 1 : at + 2, verts : 2 * verts - spare] = low[:, spare:]
    for place in range(half):
        low = [(part * half + member(place, half)) * block for part in range(2)]
        low = [wide[:, at : at + block] for at in low]
        row_s[place, 0:own_chars, 0:block] = jnp.where(side == 0, low[0], low[1])
        row_s[place, own_chars : 2 * own_chars, 0:block] = jnp.where(side == 0, low[1], low[0])
    for place in range(half):
        value = row_s[place].astype(BF16)
        for span in range(spans):
            out_ref[span * half + place] = value


def prep_kernel(
    half,
    basis_hbm,
    template_hbm,
    regressor_hbm,
    quat_hbm,
    move_hbm,
    parents_hbm,
    own_ref,
    temp_ref,
    reg_ref,
    table_ref,
    diff_ref,
    above_ref,
    shift_ref,
    basis_s,
    template_s,
    regressor_s,
    quat_raw,
    move_s,
    parents_s,
    reg_s,
    quat_s,
    parent_s,
    sems,
):
    copies = fetch(
        [
            (basis_hbm, basis_s),
            (template_hbm, template_s),
            (regressor_hbm, regressor_s),
            (quat_hbm, quat_raw),
            (move_hbm, move_s),
            (parents_hbm, parents_s),
        ],
        sems,
    )
    _, verts, block = basis_s.shape
    own_chars, _, joints = quat_raw.shape
    start, first, rest, step = layout(verts, joints)
    lane = lax.broadcasted_iota(jnp.int32, (SUBS, LANES), 1)
    sub = lax.broadcasted_iota(jnp.int32, (SUBS, LANES), 0)
    row = sub // own_chars
    char_of = sub % own_chars

    def by_char(rows):
        value = jnp.broadcast_to(rows[0], (SUBS, LANES))
        for char in range(1, own_chars):
            value = jnp.where(char_of == char, rows[char], value)
        return value

    def by_row(values):
        value = values[-1]
        for n in range(len(values) - 2, -1, -1):
            value = jnp.where(row == n, values[n], value)
        return value

    own_ref[...] = jnp.zeros_like(own_ref)
    temp_ref[...] = jnp.zeros_like(temp_ref)
    reg_s[...] = jnp.zeros_like(reg_s)
    quat_s[...] = jnp.zeros_like(quat_s)
    quat_s[:, 0:1, :] = jnp.ones_like(quat_s[:, 0:1, :])
    parent_s[...] = jnp.zeros_like(parent_s)
    for copy in copies:
        copy.wait()
    for coord in range(3):
        own_ref[coord, 0:verts, 0:block] = basis_s[coord]
    temp_ref[0:3, 0:verts] = template_s[...] * (1.0 / half)
    reg_s[start:LANES, 0:verts] = regressor_s[0:first, :]
    for coord in range(3):
        at = LANES + coord * step
        reg_s[at : at + rest, 0:verts] = regressor_s[first:joints, :]
    high, low = split_two(reg_s[...])
    for n, value in enumerate((high, low, high)):
        reg_ref[:, n * LANES : (n + 1) * LANES] = value

    quat_s[:, :, 0:joints] = quat_raw[...]
    w, x, y, z = [
        by_char([quat_s[char, comp : comp + 1, :] for char in range(own_chars)]) for comp in range(4)
    ]
    two = 2.0 / (w * w + x * x + y * y + z * z)
    rot = [
        by_row([1.0 - two * (y * y + z * z), two * (x * y + w * z), two * (x * z - w * y)]),
        by_row([two * (x * y - w * z), 1.0 - two * (x * x + z * z), two * (y * z + w * x)]),
        by_row([two * (x * z + w * y), two * (y * z - w * x), 1.0 - two * (x * x + y * y)]),
    ]
    parent_s[0:1, 0:joints] = parents_s[...]
    parent = jnp.broadcast_to(parent_s[0:1, :], (SUBS, LANES))
    parent = jnp.where((lane >= joints) | (lane == 0), joints, parent)

    wide = round_up(joints, SUBS)
    spot = lax.broadcasted_iota(jnp.int32, (wide, LANES), 0)
    target = lax.broadcasted_iota(jnp.int32, (wide, LANES), 1)
    chain = jnp.where((spot == target) & (target < joints), 1.0, 0.0)
    chain = [chain[n : n + SUBS] for n in range(0, wide, SUBS)]
    above = parent
    levels = max(1, (joints - 1).bit_length())
    for level in range(levels):
        spread = []
        for b in range(3):
            turned = [rot[b]] + [pltpu.roll(rot[b], n * own_chars, 0) for n in range(1, 4)]
            spread.append([by_row([turned[(r - m) % 4] for r in range(3)]) for m in range(3)])
        up = [pick(rot[b], above) for b in range(3)]
        rot = [sum_of([up[m] * spread[b][m] for m in range(3)]) for b in range(3)]
        chain = [value + pick(value, above) for value in chain]
        if level + 1 < levels:
            above = pick(above, above)

    for turn in range(3):
        table_ref[turn] = by_row([rot[(a + turn) % 3] for a in range(3)])
    far = jnp.zeros((SUBS, LANES), F32)
    for coord in range(3):
        diff = pick(rot[coord], parent) - rot[coord]
        diff_ref[coord] = jnp.where(lane >= start, pltpu.roll(diff, start, 1), 0.0)
        turned = pltpu.roll(diff, (coord * step - first) % LANES, 1)
        far = jnp.where((lane >= coord * step) & (lane < coord * step + rest), turned, far)
    diff_ref[3] = far
    none = jnp.zeros((SUBS, LANES), F32)
    tail = chain[first // SUBS :]
    tail = tail + [none] * (step // SUBS - len(tail))
    body = chain[: first // SUBS]
    middle = [none] * ((start - 3 * step) // SUBS)
    above_ref[...] = jnp.concatenate(tail * 3 + middle + body, axis=0).astype(BF16)
    moved = none
    for char in range(own_chars):
        for a in range(3):
            moved = jnp.where(sub == a * own_chars + char, move_s[char : char + 1, a : a + 1], moved)
    shift_ref[...] = moved


def shape_kernel(
    half,
    own_chars,
    verts,
    slots,
    joints,
    order,
    next_order,
    recv_ref,
    other_ref,
    own_ref,
    temp_ref,
    reg_ref,
    table_ref,
    out_ref,
    index_ref,
    share_ref,
    coef_ref,
    pad_s,
    skin_s,
    sum_s,
    flat_ref,
):
    block = other_ref.shape[2]
    height = 2 * own_chars + 2 * slots // half
    count = recv_ref.shape[0]
    spans = count // half
    for n in range(count):
        flat_ref[n * height : (n + 1) * height, :] = recv_ref[n].astype(F32)
    step = layout(verts, joints)[3]

    pad_s[...] = jnp.zeros_like(pad_s)
    for coord in range(3):
        pad_s[coord, 0:verts, 0:block] = other_ref[coord]
    chunk = min(16, count)
    total = own_chars * chunk
    rows_lane = lax.broadcasted_iota(jnp.int32, (total, LANES), 1)
    unit, rate = coder(verts, 2 * block)

    def do_chunk(number):
        at = number * chunk * height
        coeffs = jnp.concatenate(
            [
                jnp.concatenate(
                    [
                        flat_ref[pl.ds(at + part * own_chars + char, chunk, stride=height), :]
                        for char in range(own_chars)
                    ],
                    axis=0,
                )
                for part in range(2)
            ],
            axis=1,
        ).astype(BF16)
        shapes = [
            dot_across(coeffs, jnp.concatenate([own_ref[coord], pad_s[coord]], axis=1))
            + temp_ref[coord : coord + 1, :]
            for coord in range(3)
        ]
        high, low = split_two(jnp.concatenate(shapes, axis=0))
        sums = dot_across(jnp.concatenate([high, high, low], axis=1), reg_ref[...])
        last = sums[2 * total : 3 * total, LANES:]
        for coord in (1, 0):
            last = jnp.where(
                rows_lane < (coord + 1) * step, sums[coord * total : (coord + 1) * total, LANES:], last
            )
        rows = [shapes[coord] + sums[coord * total : (coord + 1) * total, :LANES] for coord in range(3)]
        for place, value in enumerate(rows + [last]):
            code = jnp.log2(1.0 + jnp.abs(value) * (1.0 / unit)) * (1.0 / rate)
            code = jnp.where(value < 0.0, -code, code)
            for char in range(own_chars):
                sum_s[pl.ds(number * chunk, chunk), place * own_chars + char, :] = code[
                    char * chunk : (char + 1) * chunk
                ]

    each(count // chunk, 1, do_chunk)
    for n, span in enumerate(next_order):
        at = order.index(span) * half
        out_ref[n * half : (n + 1) * half] = (
            jnp.round(sum_s[at : at + half]).astype(jnp.int32).astype(jnp.int16)
        )

    per_group = slots // half
    for base in range(0, spans, SUBS):
        many = min(SUBS, spans - base)
        rows = [None] * (2 * slots)
        for place in range(half):
            for more in range(2 * per_group):
                at = (base * half + place) * height + 2 * own_chars + more
                rows[2 * per_group * member(place, half) + more] = flat_ref[
                    pl.ds(at, many, stride=half * height), :
                ]
        spare = LANES - verts
        near = lax.broadcasted_iota(jnp.int32, (many, LANES), 1) < spare
        for n in range(0, 2 * slots, 2):
            low = jnp.where(near, pltpu.roll(rows[n], spare, 1), pltpu.roll(rows[n + 1], 2 * spare, 1))
            rows[n + 1] = rows[n + 1] + low
        scale = 1.0 / sum_of(rows[1::2])
        rows[1::2] = [value * scale for value in rows[1::2]]
        for n, value in enumerate(rows):
            skin_s[pl.ds(base * 2 * slots + n, many, stride=2 * slots), :] = value
    tiles = index_ref.shape[1] // LANES
    values = [None] * tiles
    wide_lane = lax.broadcasted_iota(jnp.int32, (2 * slots, LANES), 1)
    for span in range(spans):
        at = order.index(span) * 2 * slots
        value = skin_s[at : at + 2 * slots, :]
        low = span * verts
        value = pltpu.roll(value, low % LANES, 1) if low % LANES else value
        for tile in range(low // LANES, (low + verts - 1) // LANES + 1):
            begin = low - tile * LANES
            values[tile] = value if begin <= 0 else jnp.where(wide_lane >= begin, value, values[tile])
    for tile in range(tiles):
        at = slice(tile * LANES, (tile + 1) * LANES)
        index_ref[:, at] = values[tile].astype(jnp.int32)
        share_ref[:, at] = values[tile]
        coef = [None] * 3
        for n in range(slots):
            wide = jnp.broadcast_to(values[tile][2 * n : 2 * n + 1, :], (SUBS, LANES)).astype(jnp.int32)
            share = values[tile][2 * n + 1 : 2 * n + 2, :]
            terms = [share * pick(table_ref[part], wide) for part in range(3)]
            coef = terms if n == 0 else [coef[part] + terms[part] for part in range(3)]
        for part in range(3):
            coef_ref[part, :, at] = coef[part]


def pose_kernel(
    half,
    order,
    own_chars,
    verts,
    block,
    recv_ref,
    diff_ref,
    above_ref,
    shift_ref,
    index_ref,
    share_ref,
    coef_ref,
    out_ref,
    total_s,
):
    spans = recv_ref.shape[0] // half
    slots = index_ref.shape[0] // 2
    width = out_ref.shape[2]
    tiles = -(-width // LANES)
    lane = lax.broadcasted_iota(jnp.int32, (SUBS, LANES), 1)
    sub = lax.broadcasted_iota(jnp.int32, (SUBS, LANES), 0)
    row = sub // own_chars
    char_of = sub % own_chars
    unit, rate = coder(verts, 2 * block)

    def decode(number):
        code = recv_ref[number].astype(jnp.int32).astype(F32)
        value = jnp.exp2(jnp.abs(code) * rate) * unit - unit
        return jnp.where(code < 0.0, -value, value)

    parts = []
    shapes = [None] * tiles
    for span in range(spans):
        at = order.index(span) * half
        value = sum_of([decode(at + place) for place in range(half)])
        parts.append(value)
        low = span * verts
        turned = pltpu.roll(value, low % LANES, 1) if low % LANES else value
        for tile in range(low // LANES, (low + verts - 1) // LANES + 1):
            begin = low - tile * LANES
            shapes[tile] = turned if begin <= 0 else jnp.where(lane >= begin, turned, shapes[tile])

    total_s[...] = sum_of(parts)
    terms = []
    for coord in range(4):
        pair = jnp.broadcast_to(total_s[coord * own_chars : coord * own_chars + 1, :], (SUBS, LANES))
        for char in range(1, own_chars):
            at = coord * own_chars + char
            pair = jnp.where(char_of == char, total_s[at : at + 1, :], pair)
        terms.append(diff_ref[coord] * pair)
    lhs = (terms[0] + terms[1]) + (terms[2] + terms[3])
    high = lhs.astype(BF16).astype(F32)
    moved = dot(jnp.concatenate([high, lhs - high], axis=0).astype(BF16), above_ref[...])
    moved = (moved[:SUBS] + moved[SUBS:]) + shift_ref[...]
    for tile in range(tiles):
        end = min(width, (tile + 1) * LANES)
        at = slice(tile * LANES, (tile + 1) * LANES)
        index = [jnp.broadcast_to(index_ref[2 * n : 2 * n + 1, at], (SUBS, LANES)) for n in range(slots)]
        share = [share_ref[2 * n + 1 : 2 * n + 2, at] for n in range(slots)]
        shape = shapes[tile].astype(BF16).astype(F32)
        by_one = pltpu.roll(shape, own_chars, 0)
        by_two = pltpu.roll(shape, 2 * own_chars, 0)
        by_three = pltpu.roll(shape, 3 * own_chars, 0)
        turned = (
            coef_ref[0, :, at] * shape
            + coef_ref[1, :, at] * jnp.where(row < 2, by_three, by_two)
            + coef_ref[2, :, at] * jnp.where(row < 1, by_two, by_one)
        )
        posed = turned + sum_of([share[n] * pick(moved, index[n]) for n in range(slots)])
        for a in range(3):
            out_ref[a, :, tile * LANES : end] = posed[
                a * own_chars : (a + 1) * own_chars, : end - tile * LANES
            ].astype(BF16)


def body(spans, groups, coeffs, shape_basis, template, regressor, quaternions, translation, parents, skin_index, skin_raw):
    own_chars, comps = coeffs.shape
    verts, slots = skin_index.shape
    joints = regressor.shape[0]
    half = groups // 2
    members = spans * half
    block = comps // groups
    rows = 2 * own_chars + 2 * slots // half
    orders = (order_of(spans, spans // 2 - 1, 5), order_of(spans, spans // 2 + 1, 5))
    padded = round_up(spans * verts, LANES)
    whole = jax.ShapeDtypeStruct
    room = pltpu.CompilerParams(vmem_limit_bytes=16 * 2**20)
    basis = shape_basis.transpose(1, 2, 0)
    other = lax.ppermute(basis, "col", [(n, (n + half) % groups) for n in range(groups)])

    def exchange(value, order):
        return lax.all_to_all(
            value, ("vert", "col"), 0, 0, tiled=True, axis_index_groups=halves(groups, order)
        )

    message = pl.pallas_call(
        functools.partial(pack_kernel, groups, spans),
        out_shape=whole((members, rows, LANES), BF16),
        in_specs=[HBM] * 3,
        out_specs=VMEM,
        scratch_shapes=[
            pltpu.VMEM((own_chars, comps), BF16),
            pltpu.VMEM((slots, verts), jnp.int32),
            pltpu.VMEM((slots, verts), F32),
            pltpu.VMEM((half, rows, LANES), F32),
            pltpu.SemaphoreType.DMA((3,)),
        ],
        compiler_params=room,
        name="pack",
    )(*in_hbm(coeffs, skin_index.T, skin_raw.T))
    received = exchange(message, orders[0])
    own, temp, reg, table, *local = pl.pallas_call(
        functools.partial(prep_kernel, half),
        out_shape=[
            whole((3, LANES, LANES), BF16),
            whole((SUBS, LANES), F32),
            whole((2 * LANES, 3 * LANES), BF16),
            whole((3, SUBS, LANES), F32),
            whole((4, SUBS, LANES), F32),
            whole((LANES, LANES), BF16),
            whole((SUBS, LANES), F32),
        ],
        in_specs=[HBM] * 6,
        out_specs=[VMEM] * 7,
        scratch_shapes=[
            pltpu.VMEM((3, verts, block), BF16),
            pltpu.VMEM((3, verts), F32),
            pltpu.VMEM((joints, verts), F32),
            pltpu.VMEM((own_chars, 4, joints), F32),
            pltpu.VMEM((own_chars, 3), F32),
            pltpu.VMEM((1, joints), jnp.int32),
            pltpu.VMEM((2 * LANES, LANES), F32),
            pltpu.VMEM((own_chars, 4, LANES), F32),
            pltpu.VMEM((SUBS, LANES), jnp.int32),
            pltpu.SemaphoreType.DMA((6,)),
        ],
        compiler_params=room,
        cost_estimate=pl.CostEstimate(flops=10**7, bytes_accessed=10**6, transcendentals=0),
        name="prep",
    )(*in_hbm(basis, template, regressor, quaternions, translation, parents.reshape(1, joints)))
    partials, *skin = pl.pallas_call(
        functools.partial(shape_kernel, half, own_chars, verts, slots, joints, *orders),
        out_shape=[
            whole((members, 4 * own_chars, LANES), jnp.int16),
            whole((2 * slots, padded), jnp.int32),
            whole((2 * slots, padded), F32),
            whole((3, SUBS, padded), F32),
        ],
        in_specs=[VMEM] * 6,
        out_specs=[VMEM] * 4,
        scratch_shapes=[
            pltpu.VMEM((3, LANES, LANES), BF16),
            pltpu.VMEM((spans * 2 * slots, LANES), F32),
            pltpu.VMEM((members, 4 * own_chars, LANES), F32),
            pltpu.VMEM((members * rows, LANES), F32),
        ],
        compiler_params=room,
        name="shape",
    )(received, other, own, temp, reg, table)
    received = exchange(partials, orders[1])
    posed = pl.pallas_call(
        functools.partial(pose_kernel, half, orders[1], own_chars, verts, block),
        out_shape=whole((3, own_chars, spans * verts), BF16),
        in_specs=[VMEM] * 7,
        out_specs=VMEM,
        scratch_shapes=[pltpu.VMEM((SUBS, LANES), F32)],
        compiler_params=room,
        name="pose",
    )(received, *local, *skin)
    return posed.transpose(1, 0, 2)


def solution(mesh):
    in_specs = (
        P(("vert", "col"), None),
        P("col", None, "vert"),
        P(None, "vert"),
        P(None, "vert"),
        P(("vert", "col"), None, None),
        P(("vert", "col"), None),
        P(),
        P("vert", None),
        P("vert", None),
    )
    out_specs = P(("vert", "col"), None, None)
    return jax.shard_map(
        functools.partial(body, mesh.shape["vert"], mesh.shape["col"]),
        mesh=mesh,
        in_specs=in_specs,
        out_specs=out_specs,
        check_vma=False,
    )
```

```python
import functools
import math

import jax
import jax.numpy as jnp
from jax import lax
from jax.experimental import pallas as pl
from jax.experimental.pallas import tpu as pltpu
from jax.sharding import PartitionSpec as P

LANES = 128
SUBS = 8
VMEM = pl.BlockSpec(memory_space=pltpu.VMEM)
HBM = pl.BlockSpec(memory_space=pltpu.HBM)
F32 = jnp.float32
BF16 = jnp.bfloat16


def round_up(value, step):
    return -(-value // step) * step


def layout(verts, joints):
    start = round_up(verts, SUBS)
    first = LANES - start
    rest = joints - first
    step = round_up(rest, SUBS)
    return start, first, rest, step


def in_hbm(*values):
    return [pltpu.with_memory_space_constraint(value, pltpu.HBM) for value in values]


def split_two(value):
    high = value.astype(BF16)
    return high, (value - high.astype(F32)).astype(BF16)


def sum_of(values):
    values = list(values)
    while len(values) > 1:
        values = [sum(values[n + 1 : n + 2], values[n]) for n in range(0, len(values), 2)]
    return values[0]


def dot(lhs, rhs):
    return jnp.dot(lhs, rhs, preferred_element_type=F32)


def each(count, limit, step):
    if count <= limit:
        for number in range(count):
            step(number)
    else:
        lax.fori_loop(0, count, lambda number, carry: (step(number), carry)[1], 0)


def dot_across(lhs, rhs):
    return lax.dot_general(lhs, rhs, (((1,), (1,)), ((), ())), preferred_element_type=F32)


def pick(table, index):
    return jnp.take_along_axis(table, index, axis=1, mode="promise_in_bounds")


def fetch(pairs, sems):
    copies = [pltpu.make_async_copy(src, dst, sems.at[n]) for n, (src, dst) in enumerate(pairs)]
    for copy in copies:
        copy.start()
    return copies


def member(place, half):
    return (place + half - 1) % half


def order_of(spans, root):
    return sorted(range(spans), key=lambda n: (n != root, -abs(n - root), n))


def halves(groups, order):
    half = groups // 2
    return [
        [span * groups + side * half + member(place, half) for span in order for place in range(half)]
        for side in range(2)
    ]


def coder(verts, block):
    shape = block * 6.0 * 0.3125 + 6.0
    limit = max(shape, verts * 0.5 * shape)
    unit = 2.0**-16
    rate = math.log2(1.0 + limit / unit) / 32766.0
    return unit, rate


def pack_kernel(groups, spans, coeffs_hbm, index_hbm, raw_hbm, out_ref, coeffs_s, index_s, raw_s, row_s, sems):
    copies = fetch([(coeffs_hbm, coeffs_s), (index_hbm, index_s), (raw_hbm, raw_s)], sems)
    own_chars, comps = coeffs_s.shape
    half = groups // 2
    block = comps // groups
    slots, verts = index_s.shape
    spare = LANES - verts
    per_group = slots // half
    column = lax.rem(lax.axis_index("col"), half)
    side = lax.div(lax.axis_index("col"), half)
    row_s[...] = jnp.zeros_like(row_s)
    for copy in copies:
        copy.wait()
    wide = coeffs_s[...].astype(F32)
    index = index_s[...].astype(F32)
    raw = raw_s[...]
    for which in range(per_group):
        sel = lax.broadcasted_iota(jnp.int32, index.shape, 0) == column * per_group + which
        value = [jnp.sum(jnp.where(sel, value, 0.0), axis=0, keepdims=True) for value in (index, raw)]
        high = value[1].astype(BF16).astype(F32)
        low = value[1] - high
        at = 2 * own_chars + 2 * which
        for place in range(half):
            row_s[place, at : at + 1, 0:verts] = value[0]
            row_s[place, at : at + 1, verts:LANES] = low[:, 0:spare]
            row_s[place, at + 1 : at + 2, 0:verts] = high
            row_s[place, at + 1 : at + 2, verts : 2 * verts - spare] = low[:, spare:]
    for place in range(half):
        low = [(part * half + member(place, half)) * block for part in range(2)]
        low = [wide[:, at : at + block] for at in low]
        row_s[place, 0:own_chars, 0:block] = jnp.where(side == 0, low[0], low[1])
        row_s[place, own_chars : 2 * own_chars, 0:block] = jnp.where(side == 0, low[1], low[0])
    for place in range(half):
        value = row_s[place].astype(BF16)
        for span in range(spans):
            out_ref[span * half + place] = value


def prep_kernel(
    half,
    basis_hbm,
    template_hbm,
    regressor_hbm,
    quat_hbm,
    move_hbm,
    parents_hbm,
    own_ref,
    temp_ref,
    reg_ref,
    table_ref,
    diff_ref,
    above_ref,
    shift_ref,
    basis_s,
    template_s,
    regressor_s,
    quat_raw,
    move_s,
    parents_s,
    reg_s,
    quat_s,
    parent_s,
    sems,
):
    copies = fetch(
        [
            (basis_hbm, basis_s),
            (template_hbm, template_s),
            (regressor_hbm, regressor_s),
            (quat_hbm, quat_raw),
            (move_hbm, move_s),
            (parents_hbm, parents_s),
        ],
        sems,
    )
    _, verts, block = basis_s.shape
    own_chars, _, joints = quat_raw.shape
    start, first, rest, step = layout(verts, joints)
    lane = lax.broadcasted_iota(jnp.int32, (SUBS, LANES), 1)
    sub = lax.broadcasted_iota(jnp.int32, (SUBS, LANES), 0)
    row = sub // own_chars
    char_of = sub % own_chars

    def by_char(rows):
        value = jnp.broadcast_to(rows[0], (SUBS, LANES))
        for char in range(1, own_chars):
            value = jnp.where(char_of == char, rows[char], value)
        return value

    def by_row(values):
        value = values[-1]
        for n in range(len(values) - 2, -1, -1):
            value = jnp.where(row == n, values[n], value)
        return value

    own_ref[...] = jnp.zeros_like(own_ref)
    temp_ref[...] = jnp.zeros_like(temp_ref)
    reg_s[...] = jnp.zeros_like(reg_s)
    quat_s[...] = jnp.zeros_like(quat_s)
    quat_s[:, 0:1, :] = jnp.ones_like(quat_s[:, 0:1, :])
    parent_s[...] = jnp.zeros_like(parent_s)
    for copy in copies:
        copy.wait()
    for coord in range(3):
        own_ref[coord, 0:verts, 0:block] = basis_s[coord]
    temp_ref[0:3, 0:verts] = template_s[...] * (1.0 / half)
    reg_s[start:LANES, 0:verts] = regressor_s[0:first, :]
    for coord in range(3):
        at = LANES + coord * step
        reg_s[at : at + rest, 0:verts] = regressor_s[first:joints, :]
    high, low = split_two(reg_s[...])
    for n, value in enumerate((high, low, high)):
        reg_ref[:, n * LANES : (n + 1) * LANES] = value

    quat_s[:, :, 0:joints] = quat_raw[...]
    w, x, y, z = [
        by_char([quat_s[char, comp : comp + 1, :] for char in range(own_chars)]) for comp in range(4)
    ]
    two = 2.0 / (w * w + x * x + y * y + z * z)
    rot = [
        by_row([1.0 - two * (y * y + z * z), two * (x * y + w * z), two * (x * z - w * y)]),
        by_row([two * (x * y - w * z), 1.0 - two * (x * x + z * z), two * (y * z + w * x)]),
        by_row([two * (x * z + w * y), two * (y * z - w * x), 1.0 - two * (x * x + y * y)]),
    ]
    parent_s[0:1, 0:joints] = parents_s[...]
    parent = jnp.broadcast_to(parent_s[0:1, :], (SUBS, LANES))
    parent = jnp.where((lane >= joints) | (lane == 0), joints, parent)

    wide = round_up(joints, SUBS)
    spot = lax.broadcasted_iota(jnp.int32, (wide, LANES), 0)
    target = lax.broadcasted_iota(jnp.int32, (wide, LANES), 1)
    chain = jnp.where((spot == target) & (target < joints), 1.0, 0.0)
    chain = [chain[n : n + SUBS] for n in range(0, wide, SUBS)]
    above = parent
    levels = max(1, (joints - 1).bit_length())
    for level in range(levels):
        spread = []
        for b in range(3):
            turned = [rot[b]] + [pltpu.roll(rot[b], n * own_chars, 0) for n in range(1, 4)]
            spread.append([by_row([turned[(r - m) % 4] for r in range(3)]) for m in range(3)])
        up = [pick(rot[b], above) for b in range(3)]
        rot = [sum_of([up[m] * spread[b][m] for m in range(3)]) for b in range(3)]
        chain = [value + pick(value, above) for value in chain]
        if level + 1 < levels:
            above = pick(above, above)

    for turn in range(3):
        table_ref[turn] = by_row([rot[(a + turn) % 3] for a in range(3)])
    far = jnp.zeros((SUBS, LANES), F32)
    for coord in range(3):
        diff = pick(rot[coord], parent) - rot[coord]
        diff_ref[coord] = jnp.where(lane >= start, pltpu.roll(diff, start, 1), 0.0)
        turned = pltpu.roll(diff, (coord * step - first) % LANES, 1)
        far = jnp.where((lane >= coord * step) & (lane < coord * step + rest), turned, far)
    diff_ref[3] = far
    none = jnp.zeros((SUBS, LANES), F32)
    tail = chain[first // SUBS :]
    tail = tail + [none] * (step // SUBS - len(tail))
    body = chain[: first // SUBS]
    middle = [none] * ((start - 3 * step) // SUBS)
    above_ref[...] = jnp.concatenate(tail * 3 + middle + body, axis=0).astype(BF16)
    moved = none
    for char in range(own_chars):
        for a in range(3):
            moved = jnp.where(sub == a * own_chars + char, move_s[char : char + 1, a : a + 1], moved)
    shift_ref[...] = moved


def shape_kernel(
    half,
    own_chars,
    verts,
    slots,
    joints,
    order,
    next_order,
    recv_ref,
    other_ref,
    own_ref,
    temp_ref,
    reg_ref,
    table_ref,
    out_ref,
    index_ref,
    share_ref,
    coef_ref,
    pad_s,
    skin_s,
    sum_s,
    flat_ref,
):
    block = other_ref.shape[2]
    height = 2 * own_chars + 2 * slots // half
    count = recv_ref.shape[0]
    spans = count // half
    for n in range(count):
        flat_ref[n * height : (n + 1) * height, :] = recv_ref[n].astype(F32)
    step = layout(verts, joints)[3]

    pad_s[...] = jnp.zeros_like(pad_s)
    for coord in range(3):
        pad_s[coord, 0:verts, 0:block] = other_ref[coord]
    chunk = min(16, count)
    total = own_chars * chunk
    rows_lane = lax.broadcasted_iota(jnp.int32, (total, LANES), 1)
    unit, rate = coder(verts, 2 * block)

    def do_chunk(number):
        at = number * chunk * height
        coeffs = jnp.concatenate(
            [
                jnp.concatenate(
                    [
                        flat_ref[pl.ds(at + part * own_chars + char, chunk, stride=height), :]
                        for char in range(own_chars)
                    ],
                    axis=0,
                )
                for part in range(2)
            ],
            axis=1,
        ).astype(BF16)
        shapes = [
            dot_across(coeffs, jnp.concatenate([own_ref[coord], pad_s[coord]], axis=1))
            + temp_ref[coord : coord + 1, :]
            for coord in range(3)
        ]
        high, low = split_two(jnp.concatenate(shapes, axis=0))
        sums = dot_across(jnp.concatenate([high, high, low], axis=1), reg_ref[...])
        last = sums[2 * total : 3 * total, LANES:]
        for coord in (1, 0):
            last = jnp.where(
                rows_lane < (coord + 1) * step, sums[coord * total : (coord + 1) * total, LANES:], last
            )
        rows = [shapes[coord] + sums[coord * total : (coord + 1) * total, :LANES] for coord in range(3)]
        for place, value in enumerate(rows + [last]):
            code = jnp.log2(1.0 + jnp.abs(value) * (1.0 / unit)) * (1.0 / rate)
            code = jnp.where(value < 0.0, -code, code)
            for char in range(own_chars):
                sum_s[pl.ds(number * chunk, chunk), place * own_chars + char, :] = code[
                    char * chunk : (char + 1) * chunk
                ]

    each(count // chunk, 1, do_chunk)
    for n, span in enumerate(next_order):
        at = order.index(span) * half
        out_ref[n * half : (n + 1) * half] = (
            jnp.round(sum_s[at : at + half]).astype(jnp.int32).astype(jnp.int16)
        )

    per_group = slots // half
    for base in range(0, spans, SUBS):
        many = min(SUBS, spans - base)
        rows = [None] * (2 * slots)
        for place in range(half):
            for more in range(2 * per_group):
                at = (base * half + place) * height + 2 * own_chars + more
                rows[2 * per_group * member(place, half) + more] = flat_ref[
                    pl.ds(at, many, stride=half * height), :
                ]
        spare = LANES - verts
        near = lax.broadcasted_iota(jnp.int32, (many, LANES), 1) < spare
        for n in range(0, 2 * slots, 2):
            low = jnp.where(near, pltpu.roll(rows[n], spare, 1), pltpu.roll(rows[n + 1], 2 * spare, 1))
            rows[n + 1] = rows[n + 1] + low
        scale = 1.0 / sum_of(rows[1::2])
        rows[1::2] = [value * scale for value in rows[1::2]]
        for n, value in enumerate(rows):
            skin_s[pl.ds(base * 2 * slots + n, many, stride=2 * slots), :] = value
    tiles = index_ref.shape[1] // LANES
    values = [None] * tiles
    wide_lane = lax.broadcasted_iota(jnp.int32, (2 * slots, LANES), 1)
    for span in range(spans):
        at = order.index(span) * 2 * slots
        value = skin_s[at : at + 2 * slots, :]
        low = span * verts
        value = pltpu.roll(value, low % LANES, 1) if low % LANES else value
        for tile in range(low // LANES, (low + verts - 1) // LANES + 1):
            begin = low - tile * LANES
            values[tile] = value if begin <= 0 else jnp.where(wide_lane >= begin, value, values[tile])
    for tile in range(tiles):
        at = slice(tile * LANES, (tile + 1) * LANES)
        index_ref[:, at] = values[tile].astype(jnp.int32)
        share_ref[:, at] = values[tile]
        coef = [None] * 3
        for n in range(slots):
            wide = jnp.broadcast_to(values[tile][2 * n : 2 * n + 1, :], (SUBS, LANES)).astype(jnp.int32)
            share = values[tile][2 * n + 1 : 2 * n + 2, :]
            terms = [share * pick(table_ref[part], wide) for part in range(3)]
            coef = terms if n == 0 else [coef[part] + terms[part] for part in range(3)]
        for part in range(3):
            coef_ref[part, :, at] = coef[part]


def pose_kernel(
    half,
    order,
    own_chars,
    verts,
    block,
    recv_ref,
    diff_ref,
    above_ref,
    shift_ref,
    index_ref,
    share_ref,
    coef_ref,
    out_ref,
    total_s,
):
    spans = recv_ref.shape[0] // half
    slots = index_ref.shape[0] // 2
    width = out_ref.shape[2]
    tiles = -(-width // LANES)
    lane = lax.broadcasted_iota(jnp.int32, (SUBS, LANES), 1)
    sub = lax.broadcasted_iota(jnp.int32, (SUBS, LANES), 0)
    row = sub // own_chars
    char_of = sub % own_chars
    unit, rate = coder(verts, 2 * block)

    def decode(number):
        code = recv_ref[number].astype(jnp.int32).astype(F32)
        value = jnp.exp2(jnp.abs(code) * rate) * unit - unit
        return jnp.where(code < 0.0, -value, value)

    parts = []
    shapes = [None] * tiles
    for span in range(spans):
        at = order.index(span) * half
        value = sum_of([decode(at + place) for place in range(half)])
        parts.append(value)
        low = span * verts
        turned = pltpu.roll(value, low % LANES, 1) if low % LANES else value
        for tile in range(low // LANES, (low + verts - 1) // LANES + 1):
            begin = low - tile * LANES
            shapes[tile] = turned if begin <= 0 else jnp.where(lane >= begin, turned, shapes[tile])

    total_s[...] = sum_of(parts)
    terms = []
    for coord in range(4):
        pair = jnp.broadcast_to(total_s[coord * own_chars : coord * own_chars + 1, :], (SUBS, LANES))
        for char in range(1, own_chars):
            at = coord * own_chars + char
            pair = jnp.where(char_of == char, total_s[at : at + 1, :], pair)
        terms.append(diff_ref[coord] * pair)
    lhs = (terms[0] + terms[1]) + (terms[2] + terms[3])
    high = lhs.astype(BF16).astype(F32)
    moved = dot(jnp.concatenate([high, lhs - high], axis=0).astype(BF16), above_ref[...])
    moved = (moved[:SUBS] + moved[SUBS:]) + shift_ref[...]
    for tile in range(tiles):
        end = min(width, (tile + 1) * LANES)
        at = slice(tile * LANES, (tile + 1) * LANES)
        index = [jnp.broadcast_to(index_ref[2 * n : 2 * n + 1, at], (SUBS, LANES)) for n in range(slots)]
        share = [share_ref[2 * n + 1 : 2 * n + 2, at] for n in range(slots)]
        shape = shapes[tile].astype(BF16).astype(F32)
        by_one = pltpu.roll(shape, own_chars, 0)
        by_two = pltpu.roll(shape, 2 * own_chars, 0)
        by_three = pltpu.roll(shape, 3 * own_chars, 0)
        turned = (
            coef_ref[0, :, at] * shape
            + coef_ref[1, :, at] * jnp.where(row < 2, by_three, by_two)
            + coef_ref[2, :, at] * jnp.where(row < 1, by_two, by_one)
        )
        posed = turned + sum_of([share[n] * pick(moved, index[n]) for n in range(slots)])
        for a in range(3):
            out_ref[a, :, tile * LANES : end] = posed[
                a * own_chars : (a + 1) * own_chars, : end - tile * LANES
            ].astype(BF16)


def body(spans, groups, coeffs, shape_basis, template, regressor, quaternions, translation, parents, skin_index, skin_raw):
    own_chars, comps = coeffs.shape
    verts, slots = skin_index.shape
    joints = regressor.shape[0]
    half = groups // 2
    members = spans * half
    block = comps // groups
    rows = 2 * own_chars + 2 * slots // half
    orders = (order_of(spans, spans // 2 - 1), order_of(spans, spans // 2 + 1))
    padded = round_up(spans * verts, LANES)
    whole = jax.ShapeDtypeStruct
    room = pltpu.CompilerParams(vmem_limit_bytes=16 * 2**20)
    basis = shape_basis.transpose(1, 2, 0)
    other = lax.ppermute(basis, "col", [(n, (n + half) % groups) for n in range(groups)])

    def exchange(value, order):
        return lax.all_to_all(
            value, ("vert", "col"), 0, 0, tiled=True, axis_index_groups=halves(groups, order)
        )

    message = pl.pallas_call(
        functools.partial(pack_kernel, groups, spans),
        out_shape=whole((members, rows, LANES), BF16),
        in_specs=[HBM] * 3,
        out_specs=VMEM,
        scratch_shapes=[
            pltpu.VMEM((own_chars, comps), BF16),
            pltpu.VMEM((slots, verts), jnp.int32),
            pltpu.VMEM((slots, verts), F32),
            pltpu.VMEM((half, rows, LANES), F32),
            pltpu.SemaphoreType.DMA((3,)),
        ],
        compiler_params=room,
        name="pack",
    )(*in_hbm(coeffs, skin_index.T, skin_raw.T))
    received = exchange(message, orders[0])
    own, temp, reg, table, *local = pl.pallas_call(
        functools.partial(prep_kernel, half),
        out_shape=[
            whole((3, LANES, LANES), BF16),
            whole((SUBS, LANES), F32),
            whole((2 * LANES, 3 * LANES), BF16),
            whole((3, SUBS, LANES), F32),
            whole((4, SUBS, LANES), F32),
            whole((LANES, LANES), BF16),
            whole((SUBS, LANES), F32),
        ],
        in_specs=[HBM] * 6,
        out_specs=[VMEM] * 7,
        scratch_shapes=[
            pltpu.VMEM((3, verts, block), BF16),
            pltpu.VMEM((3, verts), F32),
            pltpu.VMEM((joints, verts), F32),
            pltpu.VMEM((own_chars, 4, joints), F32),
            pltpu.VMEM((own_chars, 3), F32),
            pltpu.VMEM((1, joints), jnp.int32),
            pltpu.VMEM((2 * LANES, LANES), F32),
            pltpu.VMEM((own_chars, 4, LANES), F32),
            pltpu.VMEM((SUBS, LANES), jnp.int32),
            pltpu.SemaphoreType.DMA((6,)),
        ],
        compiler_params=room,
        cost_estimate=pl.CostEstimate(flops=10**7, bytes_accessed=10**6, transcendentals=0),
        name="prep",
    )(*in_hbm(basis, template, regressor, quaternions, translation, parents.reshape(1, joints)))
    partials, *skin = pl.pallas_call(
        functools.partial(shape_kernel, half, own_chars, verts, slots, joints, *orders),
        out_shape=[
            whole((members, 4 * own_chars, LANES), jnp.int16),
            whole((2 * slots, padded), jnp.int32),
            whole((2 * slots, padded), F32),
            whole((3, SUBS, padded), F32),
        ],
        in_specs=[VMEM] * 6,
        out_specs=[VMEM] * 4,
        scratch_shapes=[
            pltpu.VMEM((3, LANES, LANES), BF16),
            pltpu.VMEM((spans * 2 * slots, LANES), F32),
            pltpu.VMEM((members, 4 * own_chars, LANES), F32),
            pltpu.VMEM((members * rows, LANES), F32),
        ],
        compiler_params=room,
        name="shape",
    )(received, other, own, temp, reg, table)
    received = exchange(partials, orders[1])
    posed = pl.pallas_call(
        functools.partial(pose_kernel, half, orders[1], own_chars, verts, block),
        out_shape=whole((3, own_chars, spans * verts), BF16),
        in_specs=[VMEM] * 7,
        out_specs=VMEM,
        scratch_shapes=[pltpu.VMEM((SUBS, LANES), F32)],
        compiler_params=room,
        name="pose",
    )(received, *local, *skin)
    return posed.transpose(1, 0, 2)


def solution(mesh):
    in_specs = (
        P(("vert", "col"), None),
        P("col", None, "vert"),
        P(None, "vert"),
        P(None, "vert"),
        P(("vert", "col"), None, None),
        P(("vert", "col"), None),
        P(),
        P("vert", None),
        P("vert", None),
    )
    out_specs = P(("vert", "col"), None, None)
    return jax.shard_map(
        functools.partial(body, mesh.shape["vert"], mesh.shape["col"]),
        mesh=mesh,
        in_specs=in_specs,
        out_specs=out_specs,
        check_vma=False,
    )
```
